512 devices in a mesh: rx: 4 (over y_lo, core), ry: 4 (over x), tp: 32 (over z, y_hi).
Axes of the slice: x: 4, y: 8 (y_hi: 4, y_lo: 2; y = y_hi * 2 + y_lo), z: 8, core: 2. Of those that a mesh axis runs over, the one named last changes fastest.
Arguments:
- weights: float32 [4, 4, 2, 8192, 1024], P('rx', 'ry', None, 'tp'), may hold values from -6 to 6
- factors_rx: float32 [4, 4, 2, 8, 1024], P('rx', 'ry'), may hold values from -6 to 6
- factors_ry: float32 [4, 4, 2, 8, 1024], P('rx', 'ry'), may hold values from -6 to 6
Outputs:
- mixed_weights: float32 [4, 4, 2, 8192, 1024], P('rx', 'ry', None, 'tp')
- next_rx: float32 [4, 4, 2, 8, 1024], P('rx', 'ry')
- next_ry: float32 [4, 4, 2, 8, 1024], P('rx', 'ry')
The draws below stay inside these ranges and needn't reach their ends.
All inputs are finite; a program needn't handle non-finite values.
Results may differ from the reference program's by a relative error of at most 0.00007.
Values sent between devices are 32-bit elements; how exact they have to be, the bound alone decides.
A program may use at most 64 MiB of HBM per device.

```python
import jax
import jax.numpy as jnp
from jax import lax

D = 8192
KV = 1024
RANK = 8
MATS = 2
REP_X = 4
REP_Y = 4


def steps_of(own_key, shape, cuts, low, top_value):
    def one(position, parts):
        steps = jax.random.uniform(jax.random.fold_in(jax.random.fold_in(own_key, 6), position), (parts,), jnp.float32, low / len(cuts), top_value / len(cuts))
        return jnp.repeat(jnp.exp(steps), shape[position] // parts).reshape((-1,) + (1,) * (len(shape) - position - 1))

    loudness = one(*cuts[0])
    for cut in cuts[1:]:
        loudness = loudness * one(*cut)
    return loudness


def noise(rng, dims, scale, most, split=(), kind=jnp.bfloat16):
    array = jax.random.normal(rng, dims, jnp.float32) * scale
    if len(split) > 0:
        array = steps_of(rng, dims, split, -0.22, 0.18) * array
    return jnp.clip(array, min=-most, max=most).astype(kind)


def setup_inputs(seed: int = 0) -> dict:
    arg_keys = jax.random.split(jax.random.key(seed), 4)
    weights = noise(arg_keys[0], (REP_X, REP_Y, MATS, D, KV), 1.0, 6.0, ((0, 4), (1, 4), (3, 32)), jnp.float32)
    factors_rx = noise(arg_keys[1], (REP_X, REP_Y, MATS, RANK, KV), 1.0, 6.0, ((0, 4), (1, 4)), jnp.float32)
    factors_ry = noise(arg_keys[2], (REP_X, REP_Y, MATS, RANK, KV), 1.0, 6.0, ((0, 4), (1, 4)), jnp.float32)
    return dict(weights=weights, factors_rx=factors_rx, factors_ry=factors_ry)


highest = lax.Precision.HIGHEST
mixing = 0.2

def across(values):
    return jnp.stack([jnp.roll(values[:, :, 1], -1, 0), jnp.roll(values[:, :, 0], 1, 0), jnp.roll(values[:, :, 3], -1, 1), jnp.roll(values[:, :, 2], 1, 1)], 2)

def reference(weights, factors_rx, factors_ry):
    factor_set = jnp.stack([factors_rx, jnp.roll(factors_rx, 1, 0), factors_ry, jnp.roll(factors_ry, 1, 1)], 2)
    projected = jnp.einsum('abemrk,abmdk->abemrd', factor_set, weights, precision=highest)
    differ = projected - across(projected)
    gram_sums = jnp.einsum('abemrd,abemsd->abemrs', differ, differ, precision=highest)
    lower_factor = jnp.linalg.cholesky(gram_sums)
    normalised = lax.linalg.triangular_solve(lower_factor, differ, left_side=True, lower=True)
    back_terms = jnp.einsum('abemrd,abmdk->abemrk', normalised, weights, precision=highest)
    updated = back_terms + across(back_terms)
    correction = jnp.einsum('abemrd,abemrk->abmdk', normalised, updated, precision=highest)
    mixed_weights = weights - mixing * correction
    return (mixed_weights, updated[:, :, 0], updated[:, :, 2])
```

```python
import jax
import jax.numpy as jnp
from jax import lax
from jax.experimental import pallas as pl
from jax.experimental.pallas import tpu as pltpu
from jax.sharding import PartitionSpec as P

MESH = pl.DeviceIdType.MESH
F32 = jnp.float32
BF16 = jnp.bfloat16
NZ, NY = 8, 4
FAR_FIRST = (4, 3, 5, 2, 6, 1, 7)
NT = (((1,), (1,)), ((), ()))
NN = (((1,), (0,)), ((), ()))


def split3(x):
    hi = x.astype(BF16)
    rest = x - hi.astype(F32)
    mid = rest.astype(BF16)
    low = (rest - mid.astype(F32)).astype(BF16)
    return hi, mid, low


def dot6(x, wh, wm, wl, dims):
    rows = x.shape[0]
    hi, mid, low = split3(x)
    a = lax.dot_general(jnp.concatenate([hi, mid, low], 0), wh, dims, preferred_element_type=F32)
    b = lax.dot_general(jnp.concatenate([hi, mid], 0), wm, dims, preferred_element_type=F32)
    c = lax.dot_general(hi, wl, dims, preferred_element_type=F32)
    small = (c + b[rows:]) + a[2 * rows :]
    return a[:rows] + ((a[rows : 2 * rows] + b[:rows]) + small)


def lanes_of(x):
    return x.reshape(-1, x.shape[-1])


def gossip(
    w_hbm, fx_hbm, fy_hbm, r_out, h_out,
    q, wv, wh, wm, wl, own, nb, p, c0, c1, r0, r1, g1, g2, s0, s1, q0o, q0n, q1o, q1n, f0, f1,
    local_sem, fac_s, fac_r, own_s, own_r, a0_s, a0_r, a1_s, a1_r, g1_s, g1_r, g2_s, g2_r,
    b0_s, b0_r, b0n_s, b0n_r, b1_s, b1_r, b1n_s, b1n_r, d0_s, d0_r, d1_s, d1_r, e0_s, e0_r, e1_s, e1_r,
):
    a, b, t = lax.axis_index("rx"), lax.axis_index("ry"), lax.axis_index("tp")
    z, y = t // NY, t % NY
    ap, am, bp, bm = (a + 1) % 4, (a + 3) % 4, (b + 1) % 4, (b + 3) % 4
    pa, pb = 2 * (a % 2), 2 * (b % 2)

    def owner(slot):
        par = pa if slot % 2 == 0 else pb
        return (slot + par) % 4

    par_me = jnp.where(y % 2 == 0, pa, pb)
    mine = (y + par_me) % 4
    near = [(am, b), (a, bm), (ap, b), (a, bp)]
    is_x = y % 2 == 0
    upper = mine >= 2
    my_a = jnp.where(is_x, jnp.where(upper, ap, am), a)
    my_b = jnp.where(is_x, b, jnp.where(upper, bp, bm))

    def at(ra, rb, zz, yy):
        return (ra, rb, zz * NY + yy)

    def zk(k):
        return (z + k) % NZ

    def yk(k):
        return (y + k) % NY

    def send(src, dst, ssem, rsem, dev):
        copy = pltpu.make_async_remote_copy(
            src_ref=src, dst_ref=dst, send_sem=ssem, recv_sem=rsem, device_id=dev, device_id_type=MESH
        )
        copy.start()
        return copy

    def landed(dst, rsem):
        pltpu.make_async_remote_copy(
            src_ref=dst, dst_ref=dst, send_sem=rsem, recv_sem=rsem, device_id=near_dev[0], device_id_type=MESH
        ).wait_recv()

    near_dev = [(ra, rb, t) for ra, rb in near]
    pending = []

    loads = [
        pltpu.make_async_copy(fx_hbm, q.at[2], local_sem.at[0]),
        pltpu.make_async_copy(fy_hbm, q.at[3], local_sem.at[1]),
        pltpu.make_async_copy(w_hbm.at[0], wv.at[0], local_sem.at[2]),
        pltpu.make_async_copy(w_hbm.at[1], wv.at[1], local_sem.at[3]),
    ]
    for load in loads:
        load.start()

    barrier = pltpu.get_barrier_semaphore()

    def greet(dev):
        pl.semaphore_signal(barrier, inc=1, device_id=dev, device_id_type=MESH)

    for dev in near_dev:
        greet(dev)
    for k in range(1, NZ):
        greet(at(a, b, zk(k), y))
    for k in range(1, NY):
        greet(at(a, b, z, yk(k)))
    for k in range(NY):
        greet(at(my_a, my_b, z, yk(k)))
    for k in range(NZ):
        greet(at(my_a, my_b, zk(k), y))

    for load in loads:
        load.wait()
    for m in range(2):
        hi, mid, low = split3(wv[m])
        wh[m], wm[m], wl[m] = hi, mid, low

    def project(first):
        for m in range(2):
            x = jnp.concatenate([q[first, m], q[first + 1, m]], 0)
            res = dot6(x, wh[m], wm[m], wl[m], NT)
            own[first, m] = res[:8]
            own[first + 1, m] = res[8:]

    project(2)
    pl.semaphore_wait(barrier, 4 + 7 + 3 + NY + NZ)

    pending.append(send(q.at[2], q.at[0], fac_s.at[0], fac_r.at[0], near_dev[2]))
    pending.append(send(q.at[3], q.at[1], fac_s.at[1], fac_r.at[1], near_dev[3]))
    for s in (2, 3):
        pending.append(send(own.at[s], nb.at[s ^ 2], own_s.at[s], own_r.at[s ^ 2], near_dev[s]))
    for s in (0, 1):
        landed(q.at[s], fac_r.at[s])
    project(0)
    for s in (0, 1):
        pending.append(send(own.at[s], nb.at[s ^ 2], own_s.at[s], own_r.at[s ^ 2], near_dev[s]))

    def differ(first):
        for s in (first, first + 1):
            landed(nb.at[s], own_r.at[s])
            for m in range(2):
                p[m, s] = own[s, m] - nb[s, m]

    def back(first):
        half = first // 2
        for m in range(2):
            x = lanes_of(p[m, pl.ds(first, 2)])
            res = dot6(x, wh[m], wm[m], wl[m], NN)
            for i in range(2):
                for j in range(NZ):
                    tile = res[8 * i : 8 * i + 8, 128 * j : 128 * j + 128]
                    if m == 0:
                        c0[j, first + i] = tile
                    else:
                        c1[first + i, j] = tile
            if m == 0:
                for k in FAR_FIRST:
                    part = pl.ds(first, 2)
                    pending.append(
                        send(
                            c0.at[zk(k), part], r0.at[k - 1, part],
                            a0_s.at[half, k - 1], a0_r.at[half, k - 1], at(a, b, zk(k), y),
                        )
                    )
            else:
                for s in (first, first + 1):
                    yy = owner(s)
                    k = (yy - y + NY) % NY

                    @pl.when(k != 0)
                    def _():
                        send(c1.at[s], r1.at[(k + 3) % 4], a1_s.at[s], a1_r.at[(k + 3) % 4], at(a, b, z, yy))

    differ(0)
    back(0)
    differ(2)

    rows = p[...].reshape(64, 256)
    gram = lax.dot_general(
        rows, jnp.concatenate([rows, rows], 0), NT, precision=lax.Precision.HIGHEST, preferred_element_type=F32
    )
    lane = lax.broadcasted_iota(jnp.int32, (8, 128), 1)
    block = (lane // 8) % 8
    tile = jnp.zeros((8, 128), F32)
    for i in range(8):
        tile = tile + jnp.where(block == i, gram[8 * i : 8 * i + 8], 0.0)
    g1[y] = tile
    for k in (2, 1, 3):
        pending.append(send(g1.at[y], g1.at[y], g1_s.at[k - 1], g1_r.at[k - 1], at(a, b, z, yk(k))))

    back(2)

    for k in range(1, NY):
        landed(g1.at[(y + NY - k) % NY], g1_r.at[k - 1])
    g2[z] = (g1[0] + g1[1]) + (g1[2] + g1[3])
    for k in FAR_FIRST:
        pending.append(send(g2.at[z], g2.at[z], g2_s.at[k - 1], g2_r.at[k - 1], at(a, b, zk(k), y)))

    for k in range(1, NZ):
        for half in range(2):
            landed(r0.at[k - 1, pl.ds(2 * half, 2)], a0_r.at[half, k - 1])
    total = c0[z]
    for k in range(1, NZ):
        total = total + r0[k - 1]
    s0[...] = total
    for s in range(4):
        yy = owner(s)
        k = (yy - y + NY) % NY
        pending.append(send(s0.at[s], q0n.at[y], b0n_s.at[s], b0n_r.at[y], at(*near[s], z, yy)))

        @pl.when(k != 0)
        def _():
            send(s0.at[s], q0o.at[(k + 3) % 4], b0_s.at[s], b0_r.at[(k + 3) % 4], at(a, b, z, yy))

    for k in range(1, NY):
        landed(r1.at[k - 1], a1_r.at[k - 1])
    s1[...] = (c1[mine] + r1[0]) + (r1[1] + r1[2])
    for k in FAR_FIRST:
        zz = zk(k)
        pending.append(send(s1.at[zz], q1n.at[z], b1n_s.at[k], b1n_r.at[z], at(my_a, my_b, zz, y)))
        pending.append(send(s1.at[zz], q1o.at[k - 1], b1_s.at[k - 1], b1_r.at[k - 1], at(a, b, zz, y)))
    pending.append(send(s1.at[z], q1n.at[z], b1n_s.at[0], b1n_r.at[z], at(my_a, my_b, z, y)))

    for k in range(NY):
        landed(q0n.at[k], b0n_r.at[k])
    for k in range(1, NY):
        landed(q0o.at[k - 1], b0_r.at[k - 1])
    total = (s0[mine] + q0o[0]) + (q0o[1] + q0o[2])
    f0[z, mine] = total + ((q0n[0] + q0n[1]) + (q0n[2] + q0n[3]))
    for k in (2, 1, 3):
        pending.append(
            send(f0.at[z, mine], f0.at[z, mine], d0_s.at[k - 1], d0_r.at[k - 1], at(a, b, z, yk(k)))
        )

    for k in range(NZ):
        landed(q1n.at[k], b1n_r.at[k])
    for k in range(1, NZ):
        landed(q1o.at[k - 1], b1_r.at[k - 1])
    total = s1[z]
    for k in range(1, NZ):
        total = total + q1o[k - 1]
    other = q1n[0]
    for k in range(1, NZ):
        other = other + q1n[k]
    f1[mine, z] = total + other
    for k in FAR_FIRST:
        pending.append(
            send(f1.at[mine, z], f1.at[mine, z], d1_s.at[k - 1], d1_r.at[k - 1], at(a, b, zk(k), y))
        )

    def slot_of(yy):
        return (yy + jnp.where(yy % 2 == 0, pa, pb)) % 4

    for k in range(1, NY):
        landed(f0.at[z, slot_of((y + NY - k) % NY)], d0_r.at[k - 1])
    for k in FAR_FIRST:
        pending.append(send(f0.at[z], f0.at[z], e0_s.at[k - 1], e0_r.at[k - 1], at(a, b, zk(k), y)))

    for k in range(1, NZ):
        landed(f1.at[mine, (z + NZ - k) % NZ], d1_r.at[k - 1])
    for k in (2, 1, 3):
        pending.append(send(f1.at[mine], f1.at[mine], e1_s.at[k - 1], e1_r.at[k - 1], at(a, b, z, yk(k))))

    for k in range(1, NZ):
        landed(g2.at[(z + NZ - k) % NZ], g2_r.at[k - 1])
    tile = ((g2[0] + g2[1]) + (g2[2] + g2[3])) + ((g2[4] + g2[5]) + (g2[6] + g2[7]))
    row = lax.broadcasted_iota(jnp.int32, (8, 128), 0)
    cols = [tile] + [pltpu.roll(tile, 128 - j, 1) for j in range(1, 8)]
    lower, inverse_diag = [], []
    for k in range(8):
        pivot = jnp.broadcast_to(cols[k][k : k + 1], (8, 128))
        inv = 1.0 / jnp.sqrt(pivot)
        col = cols[k] * inv
        lower.append(jnp.where(row > k, col, 0.0))
        inverse_diag.append(inv)
        for j in range(k + 1, 8):
            cols[j] = cols[j] - col * jnp.broadcast_to(col[j : j + 1], (8, 128))
    inv_cols = [jnp.where(row == j, 1.0, 0.0).astype(F32) for j in range(8)]
    for k in range(8):
        for j in range(k + 1):
            cur = inv_cols[j]
            pivot_row = jnp.broadcast_to(cur[k : k + 1], (8, 128)) * inverse_diag[k]
            cur = cur - lower[k] * pivot_row
            inv_cols[j] = jnp.where(row == k, pivot_row, cur)

    def solve(i, x):
        total = inv_cols[0][:, 8 * i : 8 * i + 1] * x[0:1]
        for j in range(1, 8):
            total = total + inv_cols[j][:, 8 * i : 8 * i + 1] * x[j : j + 1]
        return total

    for m in range(2):
        for s in range(4):
            h_out[m, s] = solve(4 * m + s, p[m, s])

    for k in range(1, NZ):
        landed(f0.at[(z + NZ - k) % NZ], e0_r.at[k - 1])
    for s in range(4):
        r_out[0, s] = solve(s, jnp.concatenate([f0[j, s] for j in range(NZ)], 1))
    for k in range(1, NY):
        landed(f1.at[slot_of((y + NY - k) % NY)], e1_r.at[k - 1])
    for s in range(4):
        r_out[1, s] = solve(4 + s, jnp.concatenate([f1[s, j] for j in range(NZ)], 1))

    for copy in pending:
        copy.wait_send()
    for s in range(4):

        @pl.when(owner(s) != y)
        def _():
            pltpu.make_async_remote_copy(
                src_ref=c1.at[s], dst_ref=c1.at[s], send_sem=a1_s.at[s], recv_sem=a1_s.at[s],
                device_id=near_dev[0], device_id_type=MESH,
            ).wait_send()
            pltpu.make_async_remote_copy(
                src_ref=s0.at[s], dst_ref=s0.at[s], send_sem=b0_s.at[s], recv_sem=b0_s.at[s],
                device_id=near_dev[0], device_id_type=MESH,
            ).wait_send()


CHUNKS = 4


def mix(w_hbm, h_ref, r_ref, out_hbm, nx_hbm, ny_hbm, wv, ov, in_sem, out_sem, small_sem):
    rows = 512 // CHUNKS

    def part(ref, i):
        return ref.at[i * rows // 256, pl.ds((i * rows) % 256, rows)]

    loads = [pltpu.make_async_copy(part(w_hbm, i), wv.at[i], in_sem.at[i]) for i in range(CHUNKS)]
    for load in loads:
        load.start()
    smalls = []
    for m in range(2):
        smalls.append(pltpu.make_async_copy(r_ref.at[m, 2], nx_hbm.at[m], small_sem.at[m]))
        smalls.append(pltpu.make_async_copy(r_ref.at[m, 3], ny_hbm.at[m], small_sem.at[2 + m]))
    for small in smalls:
        small.start()
    stores = []
    for m in range(2):
        h = h_ref[m].reshape(32, 256)
        r = r_ref[m].reshape(32, 1024)
        hh, hl, _ = split3(h)
        rh, rl, _ = split3(r)
        left = jnp.concatenate([hh, hh, hl], 0)
        right = jnp.concatenate([rh, rl, rh], 0)
        for i in range(m * CHUNKS // 2, (m + 1) * CHUNKS // 2):
            start = (i * rows) % 256
            loads[i].wait()
            term = lax.dot_general(
                left[:, start : start + rows], right, (((0,), (0,)), ((), ())), preferred_element_type=F32
            )
            ov[i] = wv[i] - 0.2 * term
            store = pltpu.make_async_copy(ov.at[i], part(out_hbm, i), out_sem.at[i])
            store.start()
            stores.append(store)
    for copy in smalls + stores:
        copy.wait()


def per_device(weights, factors_rx, factors_ry):
    w = weights.reshape(2, 256, 1024)
    vm = pltpu.VMEM
    dma = pltpu.SemaphoreType.DMA
    anyspec = pl.BlockSpec(memory_space=pl.ANY)
    vmem = pl.BlockSpec(memory_space=pltpu.VMEM)
    tile = (8, 128)
    r, h = pl.pallas_call(
        gossip,
        out_shape=(
            jax.ShapeDtypeStruct((2, 4, 8, 1024), F32),
            jax.ShapeDtypeStruct((2, 4, 8, 256), F32),
        ),
        in_specs=[anyspec] * 3,
        out_specs=(vmem, vmem),
        scratch_shapes=[
            vm((4, 2, 8, 1024), F32),
            vm((2, 256, 1024), F32),
            vm((2, 256, 1024), BF16),
            vm((2, 256, 1024), BF16),
            vm((2, 256, 1024), BF16),
            vm((4, 2, 8, 256), F32),
            vm((4, 2, 8, 256), F32),
            vm((2, 4, 8, 256), F32),
            vm((NZ, 4, *tile), F32),
            vm((4, NZ, *tile), F32),
            vm((NZ - 1, 4, *tile), F32),
            vm((NY - 1, NZ, *tile), F32),
            vm((NY, *tile), F32),
            vm((NZ, *tile), F32),
            vm((4, *tile), F32),
            vm((NZ, *tile), F32),
            vm((NY - 1, *tile), F32),
            vm((NY, *tile), F32),
            vm((NZ - 1, *tile), F32),
            vm((NZ, *tile), F32),
            vm((NZ, 4, *tile), F32),
            vm((4, NZ, *tile), F32),
            dma((4,)),
            dma((2,)), dma((2,)),
            dma((4,)), dma((4,)),
            dma((2, NZ - 1)), dma((2, NZ - 1)),
            dma((4,)), dma((NY - 1,)),
            dma((NY - 1,)), dma((NY - 1,)),
            dma((NZ - 1,)), dma((NZ - 1,)),
            dma((4,)), dma((NY - 1,)),
            dma((4,)), dma((NY,)),
            dma((NZ - 1,)), dma((NZ - 1,)),
            dma((NZ,)), dma((NZ,)),
            dma((NY - 1,)), dma((NY - 1,)),
            dma((NZ - 1,)), dma((NZ - 1,)),
            dma((NZ - 1,)), dma((NZ - 1,)),
            dma((NY - 1,)), dma((NY - 1,)),
        ],
        compiler_params=pltpu.CompilerParams(
            collective_id=0, has_side_effects=True, vmem_limit_bytes=24 * 1024 * 1024
        ),
        name="gossip",
    )(w, factors_rx.reshape(2, 8, 1024), factors_ry.reshape(2, 8, 1024))
    rows = 512 // CHUNKS
    mixed, next_rx, next_ry = pl.pallas_call(
        mix,
        out_shape=(
            jax.ShapeDtypeStruct((2, 256, 1024), F32),
            jax.ShapeDtypeStruct((2, 8, 1024), F32),
            jax.ShapeDtypeStruct((2, 8, 1024), F32),
        ),
        in_specs=[anyspec, vmem, vmem],
        out_specs=(anyspec, anyspec, anyspec),
        scratch_shapes=[
            vm((CHUNKS, rows, 1024), F32),
            vm((CHUNKS, rows, 1024), F32),
            dma((CHUNKS,)),
            dma((CHUNKS,)),
            dma((4,)),
        ],
        compiler_params=pltpu.CompilerParams(vmem_limit_bytes=24 * 1024 * 1024),
        name="mix",
    )(w, h, r)
    return (
        mixed.reshape(1, 1, 2, 256, 1024),
        next_rx.reshape(1, 1, 2, 8, 1024),
        next_ry.reshape(1, 1, 2, 8, 1024),
    )


def solution(mesh):
    wide = P("rx", "ry", None, "tp", None)
    narrow = P("rx", "ry", None, None, None)
    return jax.shard_map(
        per_device, mesh=mesh, in_specs=(wide, narrow, narrow), out_specs=(wide, narrow, narrow), check_vma=False
    )
```

```python
import jax
import jax.numpy as jnp
from jax import lax
from jax.experimental import pallas as pl
from jax.experimental.pallas import tpu as pltpu
from jax.sharding import PartitionSpec as P

MESH = pl.DeviceIdType.MESH
F32 = jnp.float32
BF16 = jnp.bfloat16
NZ, NY = 8, 4
Z_ORDER = (4, 3, 5, 2, 6, 1, 7, 0)
NT = (((1,), (1,)), ((), ()))
NN = (((1,), (0,)), ((), ()))


def split3(x):
    hi = x.astype(BF16)
    rest = x - hi.astype(F32)
    mid = rest.astype(BF16)
    low = (rest - mid.astype(F32)).astype(BF16)
    return hi, mid, low


def dot6(x, wh, wm, wl, dims):
    rows = x.shape[0]
    hi, mid, low = split3(x)
    a = lax.dot_general(jnp.concatenate([hi, mid, low], 0), wh, dims, preferred_element_type=F32)
    b = lax.dot_general(jnp.concatenate([hi, mid], 0), wm, dims, preferred_element_type=F32)
    c = lax.dot_general(hi, wl, dims, preferred_element_type=F32)
    small = (c + b[rows:]) + a[2 * rows :]
    return a[:rows] + ((a[rows : 2 * rows] + b[:rows]) + small)


def gossip(
    w_hbm, fx_hbm, fy_hbm, r_out, h_out,
    q, wv, wh, wm, wl, own, nb, p, c, inbox, g1, g2, f,
    load_sem, fac_s, fac_r, own_s, own_r, sum_s, sum_r, all_s, all_r, g1_s, g1_r, g2_s, g2_r, heard,
):
    a, b, t = lax.axis_index("rx"), lax.axis_index("ry"), lax.axis_index("tp")
    z, y = t // NY, t % NY
    zs = [(z + k) % NZ for k in range(NZ)]
    ys = [(y + k) % NY for k in range(NY)]
    near = [((a + 3) % 4, b), (a, (b + 3) % 4), ((a + 1) % 4, b), (a, (b + 1) % 4)]
    turn = [2 * (a % 2), 2 * (b % 2)]
    owner = [(slot + turn[slot % 2]) % NY for slot in range(4)]
    from_owner = [(y + NY - owner[slot]) % NY for slot in range(4)]
    mine = (y + jnp.where(y % 2 == 0, turn[0], turn[1])) % 4
    step = jnp.where(mine >= 2, 1, 3)
    far_a = jnp.where(y % 2 == 0, (a + step) % 4, a)
    far_b = jnp.where(y % 2 == 0, b, (b + step) % 4)
    my_matrix = jnp.where(mine >= 2, 0, 1)
    my_tile = my_matrix * 32 + mine * NZ + z
    far_tile = my_matrix * 32 + ((mine + 2) % 4) * NZ + z

    def at(zz, yy):
        return (a, b, zz * NY + yy)

    def send(src, dst, ssem, rsem, dev):
        pltpu.make_async_remote_copy(
            src_ref=src, dst_ref=dst, send_sem=ssem, recv_sem=rsem, device_id=dev, device_id_type=MESH
        ).start()

    def counted(ref, sem):
        return pltpu.make_async_remote_copy(
            src_ref=ref, dst_ref=ref, send_sem=sem, recv_sem=sem, device_id=near_dev[0], device_id_type=MESH
        )

    near_dev = [(ra, rb, t) for ra, rb in near]

    loads = []
    for m in range(2):
        loads.append(pltpu.make_async_copy(fx_hbm.at[m], q.at[m, 2], load_sem.at[m]))
        loads.append(pltpu.make_async_copy(fy_hbm.at[m], q.at[m, 3], load_sem.at[2 + m]))
    for m in range(2):
        loads.append(pltpu.make_async_copy(w_hbm.at[m], wv.at[m], load_sem.at[4 + m]))
    for load in loads:
        load.start()

    beside = [at(zs[1], y), at(zs[7], y)]
    across = [at(z, ys[1]), at(z, ys[3])]
    barrier = pltpu.get_barrier_semaphore()
    for dev in near_dev + beside + across:
        pl.semaphore_signal(barrier, inc=1, device_id=dev, device_id_type=MESH)
    rounds = [beside + across, beside + across, beside, [at(zs[2], y), at(zs[6], y)], beside]

    def tell(i):
        for dev in rounds[i]:
            pl.semaphore_signal(heard.at[i], inc=1, device_id=dev, device_id_type=MESH)

    def hear(i):
        pl.semaphore_wait(heard.at[i], len(rounds[i]))

    pl.semaphore_wait(barrier, 8)
    tell(0)
    for m in range(2):
        for s in (2, 3):
            loads[2 * m + s - 2].wait()
            send(q.at[m, s], q.at[m, s - 2], fac_s, fac_r.at[m], near_dev[s])

    def project(first, m):
        x = q[m, pl.ds(first, 2)].reshape(16, 1024)
        res = dot6(x, wh[m], wm[m], wl[m], NT)
        for i in range(2):
            own[m, first + i] = res[8 * i : 8 * i + 8]
        for s in (first, first + 1):
            send(own.at[m, s], nb.at[m, s ^ 2], own_s, own_r.at[1 - first // 2, m], near_dev[s])

    for m in range(2):
        loads[4 + m].wait()
        hi, mid, low = split3(wv[m])
        wh[m], wm[m], wl[m] = hi, mid, low
    hear(0)
    tell(1)
    for m in range(2):
        project(2, m)
    hear(1)
    tell(2)
    for m in range(2):
        counted(q.at[m, pl.ds(0, 2)], fac_r.at[m]).wait_recv()
        project(0, m)
        if m == 0:
            hear(2)
            tell(3)
    hear(3)
    tell(4)

    def differ(first, m):
        part = pl.ds(first, 2)
        counted(nb.at[m, part], own_r.at[first // 2, m]).wait_recv()
        p[m, part] = own[m, part] - nb[m, part]

    def back(first, m):
        x = p[m, pl.ds(first, 2)].reshape(16, 256)
        res = dot6(x, wh[m], wm[m], wl[m], NN)
        for i in range(2):
            for j in range(NZ):
                c[m * 32 + (first + i) * NZ + j] = res[8 * i : 8 * i + 8, 128 * j : 128 * j + 128]

    def share(first, m):
        here = m == (0 if first == 2 else 1)
        for k in Z_ORDER:
            for s in (first, first + 1):
                src = c.at[m * 32 + s * NZ + zs[k]]
                slot = ((NZ - k) % NZ) * NY + from_owner[s] + (0 if here else 32)
                ra, rb = (a, b) if here else near[s]
                dev = (ra, rb, zs[k] * NY + owner[s])
                if here and k == 0:

                    @pl.when(owner[s] != y)
                    def _():
                        send(src, inbox.at[slot], sum_s, sum_r, dev)
                else:
                    send(src, inbox.at[slot], sum_s, sum_r, dev)

    for m in range(2):
        differ(0, m)
        back(0, m)
    hear(4)
    for m in range(2):
        share(0, m)
    for m in range(2):
        differ(2, m)
        back(2, m)
        share(2, m)

    rows = p[...].reshape(64, 256)
    gram = lax.dot_general(
        rows, jnp.concatenate([rows, rows], 0), NT, precision=lax.Precision.HIGHEST, preferred_element_type=F32
    )
    lane = lax.broadcasted_iota(jnp.int32, (8, 128), 1)
    block = (lane // 8) % 8
    tile = jnp.zeros((8, 128), F32)
    for i in range(8):
        tile = tile + jnp.where(block == i, gram[8 * i : 8 * i + 8], 0.0)
    g1[y] = tile
    for k in (2, 1, 3):
        send(g1.at[y], g1.at[y], g1_s, g1_r, at(z, ys[k]))
    counted(g1.at[pl.ds(0, NY - 1)], g1_r).wait_recv()
    g2[z] = (g1[0] + g1[1]) + (g1[2] + g1[3])
    for k in Z_ORDER[:-1]:
        send(g2.at[z], g2.at[z], g2_s, g2_r, at(zs[k], y))

    counted(inbox.at[pl.ds(1, 63)], sum_r).wait_recv()
    parts = [c[my_tile], inbox[1], inbox[2], inbox[3]]
    for i in range(4, 64):
        parts[i % 4] = parts[i % 4] + inbox[i]
    f[my_tile] = (parts[0] + parts[1]) + (parts[2] + parts[3])
    ordered = [(k, j) for k in range(NZ) for j in range(NY)]
    ordered.sort(key=lambda kj: -(min(kj[0], NZ - kj[0]) + 2 * min(kj[1], NY - kj[1])))
    for k, j in ordered:
        there = zs[k] * NY + ys[j]
        send(f.at[my_tile], f.at[far_tile], all_s, all_r, (far_a, far_b, there))
        if k or j:
            send(f.at[my_tile], f.at[my_tile], all_s, all_r, (a, b, there))

    counted(g2.at[pl.ds(0, NZ - 1)], g2_r).wait_recv()
    tile = ((g2[0] + g2[1]) + (g2[2] + g2[3])) + ((g2[4] + g2[5]) + (g2[6] + g2[7]))
    row = lax.broadcasted_iota(jnp.int32, (8, 128), 0)
    cols = [tile] + [pltpu.roll(tile, 128 - j, 1) for j in range(1, 8)]
    lower, inverse_diag = [], []
    for k in range(8):
        pivot = jnp.broadcast_to(cols[k][k : k + 1], (8, 128))
        inv = 1.0 / jnp.sqrt(pivot)
        col = cols[k] * inv
        lower.append(jnp.where(row > k, col, 0.0))
        inverse_diag.append(inv)
        for j in range(k + 1, 8):
            cols[j] = cols[j] - col * jnp.broadcast_to(col[j : j + 1], (8, 128))
    inv_cols = [jnp.where(row == j, 1.0, 0.0).astype(F32) for j in range(8)]
    for k in range(8):
        for j in range(k + 1):
            cur = inv_cols[j]
            pivot_row = jnp.broadcast_to(cur[k : k + 1], (8, 128)) * inverse_diag[k]
            cur = cur - lower[k] * pivot_row
            inv_cols[j] = jnp.where(row == k, pivot_row, cur)

    def solve(i, x):
        total = inv_cols[0][:, 8 * i : 8 * i + 1] * x[0:1]
        for j in range(1, 8):
            total = total + inv_cols[j][:, 8 * i : 8 * i + 1] * x[j : j + 1]
        return total

    for m in range(2):
        for s in range(4):
            h_out[m, s] = solve(4 * m + s, p[m, s])

    counted(f.at[pl.ds(0, 63)], all_r).wait_recv()
    for m in range(2):
        for s in range(4):
            r_out[m, s] = solve(4 * m + s, jnp.concatenate([f[m * 32 + s * NZ + j] for j in range(NZ)], 1))

    counted(q.at[pl.ds(0, 2), pl.ds(2, 2)], fac_s).wait_send()
    counted(own, own_s).wait_send()
    counted(c.at[pl.ds(0, 63)], sum_s).wait_send()
    counted(f.at[pl.ds(0, 63)], all_s).wait_send()
    counted(g1.at[pl.ds(0, NY - 1)], g1_s).wait_send()
    counted(g2.at[pl.ds(0, NZ - 1)], g2_s).wait_send()


CHUNKS = 4


def mix(w_ref, h_ref, r_ref, out_hbm, nx_hbm, ny_hbm, ov, out_sem, small_sem):
    rows = 512 // CHUNKS
    stores = []
    for m in range(2):
        stores.append(pltpu.make_async_copy(r_ref.at[m, 2], nx_hbm.at[m], small_sem.at[m]))
        stores.append(pltpu.make_async_copy(r_ref.at[m, 3], ny_hbm.at[m], small_sem.at[2 + m]))
    for store in stores:
        store.start()
    for m in range(2):
        h = h_ref[m].reshape(32, 256)
        r = r_ref[m].reshape(32, 1024)
        hh, hl, _ = split3(h)
        rh, rl, _ = split3(r)
        left = jnp.concatenate([hh, hh, hl], 0)
        right = jnp.concatenate([rh, rl, rh], 0)
        for i in range(m * CHUNKS // 2, (m + 1) * CHUNKS // 2):
            start = (i * rows) % 256
            term = lax.dot_general(
                left[:, start : start + rows], right, (((0,), (0,)), ((), ())), preferred_element_type=F32
            )
            ov[i] = w_ref[m, start : start + rows] - 0.2 * term
            store = pltpu.make_async_copy(ov.at[i], out_hbm.at[m, pl.ds(start, rows)], out_sem.at[i])
            store.start()
            stores.append(store)
    for store in stores:
        store.wait()


def per_device(weights, factors_rx, factors_ry):
    w = weights.reshape(2, 256, 1024)
    vm = pltpu.VMEM
    dma = pltpu.SemaphoreType.DMA
    anyspec = pl.BlockSpec(memory_space=pl.ANY)
    hbm = pl.BlockSpec(memory_space=pltpu.HBM)
    vmem = pl.BlockSpec(memory_space=pltpu.VMEM)
    tile = (8, 128)
    r, h = pl.pallas_call(
        gossip,
        out_shape=(
            jax.ShapeDtypeStruct((2, 4, 8, 1024), F32),
            jax.ShapeDtypeStruct((2, 4, 8, 256), F32),
        ),
        in_specs=[hbm] * 3,
        out_specs=(vmem, vmem),
        scratch_shapes=[
            vm((2, 4, 8, 1024), F32),
            vm((2, 256, 1024), F32),
            vm((2, 256, 1024), BF16),
            vm((2, 256, 1024), BF16),
            vm((2, 256, 1024), BF16),
            vm((2, 4, 8, 256), F32),
            vm((2, 4, 8, 256), F32),
            vm((2, 4, 8, 256), F32),
            vm((64, *tile), F32),
            vm((64, *tile), F32),
            vm((NY, *tile), F32),
            vm((NZ, *tile), F32),
            vm((64, *tile), F32),
            dma((6,)),
            dma, dma((2,)),
            dma, dma((2, 2)),
            dma, dma,
            dma, dma,
            dma, dma,
            dma, dma,
            pltpu.SemaphoreType.REGULAR((5,)),
        ],
        compiler_params=pltpu.CompilerParams(
            collective_id=0, has_side_effects=True, vmem_limit_bytes=24 * 1024 * 1024
        ),
        name="gossip",
    )(*[pltpu.with_memory_space_constraint(x, pltpu.HBM) for x in (w, factors_rx.reshape(2, 8, 1024), factors_ry.reshape(2, 8, 1024))])
    rows = 512 // CHUNKS
    mixed, next_rx, next_ry = pl.pallas_call(
        mix,
        out_shape=(
            jax.ShapeDtypeStruct((2, 256, 1024), F32),
            jax.ShapeDtypeStruct((2, 8, 1024), F32),
            jax.ShapeDtypeStruct((2, 8, 1024), F32),
        ),
        in_specs=[vmem, vmem, vmem],
        out_specs=(anyspec, anyspec, anyspec),
        scratch_shapes=[
            vm((CHUNKS, rows, 1024), F32),
            dma((CHUNKS,)),
            dma((4,)),
        ],
        compiler_params=pltpu.CompilerParams(vmem_limit_bytes=24 * 1024 * 1024),
        name="mix",
    )(w, h, r)
    return (
        mixed.reshape(1, 1, 2, 256, 1024),
        next_rx.reshape(1, 1, 2, 8, 1024),
        next_ry.reshape(1, 1, 2, 8, 1024),
    )


def solution(mesh):
    wide = P("rx", "ry", None, "tp", None)
    narrow = P("rx", "ry", None, None, None)
    return jax.shard_map(
        per_device, mesh=mesh, in_specs=(wide, narrow, narrow), out_specs=(wide, narrow, narrow), check_vma=False
    )
```

```python
import jax
import jax.numpy as jnp
from jax import lax
from jax.experimental import pallas as pl
from jax.experimental.pallas import tpu as pltpu
from jax.sharding import PartitionSpec as P

MESH = pl.DeviceIdType.MESH
F32 = jnp.float32
BF16 = jnp.bfloat16
NZ, NY = 8, 4
Z_ORDER = (4, 5, 3, 6, 2, 7, 1, 0)
NT = (((1,), (1,)), ((), ()))
NN = (((1,), (0,)), ((), ()))


def split3(x):
    hi = x.astype(BF16)
    rest = x - hi.astype(F32)
    mid = rest.astype(BF16)
    low = (rest - mid.astype(F32)).astype(BF16)
    return hi, mid, low


def dot6(x, wh, wm, wl, dims):
    rows = x.shape[0]
    hi, mid, low = split3(x)
    a = lax.dot_general(jnp.concatenate([hi, mid, low], 0), wh, dims, preferred_element_type=F32)
    b = lax.dot_general(jnp.concatenate([hi, mid], 0), wm, dims, preferred_element_type=F32)
    c = lax.dot_general(hi, wl, dims, preferred_element_type=F32)
    small = (c + b[rows:]) + a[2 * rows :]
    return a[:rows] + ((a[rows : 2 * rows] + b[:rows]) + small)


def spread():
    far_first = lambda kj: -(min(kj[0], NZ - kj[0]) + min(kj[1], NY - kj[1]))
    sides = [
        sorted([(k, j) for k in side for j in range(NY)], key=far_first)
        for side in (range(1, 5), range(5, NZ), range(1))
    ]
    order = [((i + 0.5) / len(side), n, kj) for n, side in enumerate(sides) for i, kj in enumerate(side)]
    return [kj for _, _, kj in sorted(order)]


def gossip(
    w_hbm, fx_hbm, fy_hbm, r_out, h_out,
    q, wv, wh, wm, wl, own, nb, p, c, inbox, g1, g2, f,
    load_sem, fac_s, fac_r, own_s, own_r, sum_s, sum_r, all_s, all_r, g1_s, g1_r, g2_s, g2_r, heard,
):
    a, b, t = lax.axis_index("rx"), lax.axis_index("ry"), lax.axis_index("tp")
    z, y = lax.div(t, NY), lax.rem(t, NY)
    zs = [lax.rem(z + k, NZ) for k in range(NZ)]
    ys = [lax.rem(y + k, NY) for k in range(NY)]
    near = [(lax.rem(a + 3, 4), b), (a, lax.rem(b + 3, 4)), (lax.rem(a + 1, 4), b), (a, lax.rem(b + 1, 4))]
    near_dev = [(ra, rb, t) for ra, rb in near]

    def at(zz, yy):
        return (a, b, zz * NY + yy)

    beside = [at(zs[1], y), at(zs[7], y)]
    across = [at(z, ys[1]), at(z, ys[3])]
    barrier = pltpu.get_barrier_semaphore()
    for dev in near_dev + beside + across:
        pl.semaphore_signal(barrier, inc=1, device_id=dev, device_id_type=MESH)
    rounds = [across + beside, across + [at(zs[2], y), at(zs[6], y)], [at(zs[k], y) for k in Z_ORDER[:-1]]]

    def tell(i):
        for dev in rounds[i]:
            pl.semaphore_signal(heard.at[i], inc=1, device_id=dev, device_id_type=MESH)

    def hear(i):
        pl.semaphore_wait(heard.at[i], len(rounds[i]))

    def send(src, dst, ssem, rsem, dev):
        pltpu.make_async_remote_copy(
            src_ref=src, dst_ref=dst, send_sem=ssem, recv_sem=rsem, device_id=dev, device_id_type=MESH
        ).start()

    def counted(ref, sem):
        return pltpu.make_async_remote_copy(
            src_ref=ref, dst_ref=ref, send_sem=sem, recv_sem=sem, device_id=near_dev[0], device_id_type=MESH
        )

    loads = [
        pltpu.make_async_copy(fx_hbm, q.at[2], load_sem.at[0]),
        pltpu.make_async_copy(fy_hbm, q.at[3], load_sem.at[1]),
        pltpu.make_async_copy(w_hbm.at[0], wv.at[0], load_sem.at[2]),
        pltpu.make_async_copy(w_hbm.at[1], wv.at[1], load_sem.at[3]),
    ]
    for load in loads:
        load.start()

    turn = [2 * lax.rem(a, 2), 2 * lax.rem(a + b, 2)]
    owner = [lax.rem(slot + turn[slot % 2], NY) for slot in range(4)]
    from_owner = [lax.rem(y + NY - owner[slot], NY) for slot in range(4)]
    odd = lax.rem(y, 2)
    mine = lax.rem(y + (1 - odd) * turn[0] + odd * turn[1], NY)
    step = 3 - 2 * lax.div(mine, 2)
    far_a, far_b = lax.rem(a + (1 - odd) * step, 4), lax.rem(b + odd * step, 4)
    my_matrix = 1 - lax.div(mine, 2)
    my_tile = (mine * NZ + z) * 2 + my_matrix
    far_tile = (lax.rem(mine + 2, 4) * NZ + z) * 2 + my_matrix

    pl.semaphore_wait(barrier, 8)
    tell(0)
    for s in (2, 3):
        loads[s - 2].wait()
        send(q.at[s], q.at[s - 2], fac_s, fac_r, near_dev[s])

    def project(first):
        for m in range(2):
            x = q[pl.ds(first, 2), m].reshape(16, 1024)
            res = dot6(x, wh[m], wm[m], wl[m], NT)
            for i in range(2):
                own[first + i, m] = res[8 * i : 8 * i + 8]
        for s in (first, first + 1):
            send(own.at[s], nb.at[s ^ 2], own_s, own_r.at[1 - first // 2], near_dev[s])

    def differ(first):
        part = pl.ds(first, 2)
        counted(nb.at[part], own_r.at[first // 2]).wait_recv()
        p[part] = own[part] - nb[part]

    def back(first, m):
        x = p[pl.ds(first, 2), m].reshape(16, 256)
        res = dot6(x, wh[m], wm[m], wl[m], NN)
        for i in range(2):
            for j in range(NZ):
                c[((first + i) * NZ + j) * 2 + m] = res[8 * i : 8 * i + 8, 128 * j : 128 * j + 128]

    def share(first, m, order):
        here = m == 1 - first // 2
        for k in order:
            for s in (first, first + 1):
                src = c.at[(s * NZ + zs[k]) * 2 + m]
                dst = inbox.at[((NZ - k) % NZ) * NY + from_owner[s] + (0 if here else 32)]
                ra, rb = (a, b) if here else near[s]
                dev = (ra, rb, zs[k] * NY + owner[s])
                if here and k == 0:

                    @pl.when(owner[s] != y)
                    def _():
                        send(src, dst, sum_s, sum_r, dev)
                else:
                    send(src, dst, sum_s, sum_r, dev)

    for m in range(2):
        loads[2 + m].wait()
        hi, mid, low = split3(wv[m])
        wh[m], wm[m], wl[m] = hi, mid, low
    project(2)
    hear(0)
    tell(1)
    counted(q.at[pl.ds(0, 2)], fac_r).wait_recv()
    hear(1)
    tell(2)
    project(0)
    differ(0)
    for m in range(2):
        back(0, m)
    hear(2)
    share(0, 0, Z_ORDER)
    share(0, 1, Z_ORDER[:3])
    differ(2)
    back(2, 0)
    share(2, 0, Z_ORDER)
    back(2, 1)
    share(2, 1, Z_ORDER[:3])

    rows = p[...].reshape(64, 256)
    gram = lax.dot_general(
        rows, jnp.concatenate([rows, rows], 0), NT, precision=lax.Precision.HIGHEST, preferred_element_type=F32
    )
    lane = lax.broadcasted_iota(jnp.int32, (8, 128), 1)
    block = (lane // 8) % 8
    tile = jnp.zeros((8, 128), F32)
    for i in range(8):
        tile = tile + jnp.where(block == i, gram[8 * i : 8 * i + 8], 0.0)
    g1[y] = tile
    for k in (2, 1, 3):
        send(g1.at[y], g1.at[y], g1_s, g1_r, at(z, ys[k]))
    for k in Z_ORDER[3:]:
        share(0, 1, (k,))
        share(2, 1, (k,))
    counted(g1.at[pl.ds(0, NY - 1)], g1_r).wait_recv()
    g2[z] = (g1[0] + g1[1]) + (g1[2] + g1[3])
    for k in Z_ORDER[:-1]:
        send(g2.at[z], g2.at[z], g2_s, g2_r, at(zs[k], y))

    counted(inbox.at[pl.ds(1, 63)], sum_r).wait_recv()
    parts = [c[my_tile], inbox[1], inbox[2], inbox[3]]
    for i in range(4, 64):
        parts[i % 4] = parts[i % 4] + inbox[i]
    f[my_tile] = (parts[0] + parts[1]) + (parts[2] + parts[3])
    for k, j in spread():
        there = zs[k] * NY + ys[j]
        send(f.at[my_tile], f.at[far_tile], all_s, all_r, (far_a, far_b, there))
        if k or j:
            send(f.at[my_tile], f.at[my_tile], all_s, all_r, (a, b, there))

    counted(g2.at[pl.ds(0, NZ - 1)], g2_r).wait_recv()
    tile = ((g2[0] + g2[1]) + (g2[2] + g2[3])) + ((g2[4] + g2[5]) + (g2[6] + g2[7]))
    row = lax.broadcasted_iota(jnp.int32, (8, 128), 0)
    cols = [tile] + [pltpu.roll(tile, 128 - j, 1) for j in range(1, 8)]
    lower, inverse_diag = [], []
    for k in range(8):
        pivot = jnp.broadcast_to(cols[k][k : k + 1], (8, 128))
        inv = 1.0 / jnp.sqrt(pivot)
        col = cols[k] * inv
        lower.append(jnp.where(row > k, col, 0.0))
        inverse_diag.append(inv)
        for j in range(k + 1, 8):
            cols[j] = cols[j] - col * jnp.broadcast_to(col[j : j + 1], (8, 128))
    inv_cols = [jnp.where(row == j, 1.0, 0.0).astype(F32) for j in range(8)]
    for k in range(8):
        for j in range(k + 1):
            cur = inv_cols[j]
            pivot_row = jnp.broadcast_to(cur[k : k + 1], (8, 128)) * inverse_diag[k]
            cur = cur - lower[k] * pivot_row
            inv_cols[j] = jnp.where(row == k, pivot_row, cur)

    def solve(i, x):
        total = inv_cols[0][:, 8 * i : 8 * i + 1] * x[0:1]
        for j in range(1, 8):
            total = total + inv_cols[j][:, 8 * i : 8 * i + 1] * x[j : j + 1]
        return total

    for m in range(2):
        for s in range(4):
            h_out[m, s] = solve(2 * s + m, p[s, m])

    counted(f.at[pl.ds(0, 63)], all_r).wait_recv()
    for m in range(2):
        for s in range(4):
            r_out[m, s] = solve(2 * s + m, jnp.concatenate([f[(s * NZ + j) * 2 + m] for j in range(NZ)], 1))

    counted(q.at[pl.ds(2, 2)], fac_s).wait_send()
    counted(own, own_s).wait_send()
    counted(c.at[pl.ds(0, 63)], sum_s).wait_send()
    counted(f.at[pl.ds(0, 63)], all_s).wait_send()
    counted(g1.at[pl.ds(0, NY - 1)], g1_s).wait_send()
    counted(g2.at[pl.ds(0, NZ - 1)], g2_s).wait_send()


CHUNKS = 8


def mix(w_ref, h_ref, r_ref, out_hbm, nx_hbm, ny_hbm, ov, out_sem, small_sem):
    rows = 512 // CHUNKS
    stores = []
    for m in range(2):
        stores.append(pltpu.make_async_copy(r_ref.at[m, 2], nx_hbm.at[m], small_sem.at[m]))
        stores.append(pltpu.make_async_copy(r_ref.at[m, 3], ny_hbm.at[m], small_sem.at[2 + m]))
    for store in stores:
        store.start()
    for m in range(2):
        h = h_ref[m].reshape(32, 256)
        r = r_ref[m].reshape(32, 1024)
        hh, hl, _ = split3(h)
        rh, rl, _ = split3(r)
        left = jnp.concatenate([hh, hh, hl], 0)
        right = jnp.concatenate([rh, rl, rh], 0)
        for i in range(m * CHUNKS // 2, (m + 1) * CHUNKS // 2):
            start = (i * rows) % 256
            term = lax.dot_general(
                left[:, start : start + rows], right, (((0,), (0,)), ((), ())), preferred_element_type=F32
            )
            ov[i] = w_ref[m, start : start + rows] - 0.2 * term
            store = pltpu.make_async_copy(ov.at[i], out_hbm.at[m, pl.ds(start, rows)], out_sem.at[i])
            store.start()
            stores.append(store)
    for store in stores:
        store.wait()


def per_device(weights, factors_rx, factors_ry):
    w = weights.reshape(2, 256, 1024)
    vm = pltpu.VMEM
    dma = pltpu.SemaphoreType.DMA
    anyspec = pl.BlockSpec(memory_space=pl.ANY)
    hbm = pl.BlockSpec(memory_space=pltpu.HBM)
    vmem = pl.BlockSpec(memory_space=pltpu.VMEM)
    tile = (8, 128)
    r, h = pl.pallas_call(
        gossip,
        out_shape=(
            jax.ShapeDtypeStruct((2, 4, 8, 1024), F32),
            jax.ShapeDtypeStruct((2, 4, 8, 256), F32),
        ),
        in_specs=[hbm] * 3,
        out_specs=(vmem, vmem),
        scratch_shapes=[
            vm((4, 2, 8, 1024), F32),
            vm((2, 256, 1024), F32),
            vm((2, 256, 1024), BF16),
            vm((2, 256, 1024), BF16),
            vm((2, 256, 1024), BF16),
            vm((4, 2, 8, 256), F32),
            vm((4, 2, 8, 256), F32),
            vm((4, 2, 8, 256), F32),
            vm((64, *tile), F32),
            vm((64, *tile), F32),
            vm((NY, *tile), F32),
            vm((NZ, *tile), F32),
            vm((64, *tile), F32),
            dma((4,)),
            dma, dma,
            dma, dma((2,)),
            dma, dma,
            dma, dma,
            dma, dma,
            dma, dma,
            pltpu.SemaphoreType.REGULAR((3,)),
        ],
        compiler_params=pltpu.CompilerParams(
            collective_id=0, has_side_effects=True, vmem_limit_bytes=24 * 1024 * 1024
        ),
        name="gossip",
    )(*[pltpu.with_memory_space_constraint(x, pltpu.HBM) for x in (w, factors_rx.reshape(2, 8, 1024), factors_ry.reshape(2, 8, 1024))])
    rows = 512 // CHUNKS
    mixed, next_rx, next_ry = pl.pallas_call(
        mix,
        out_shape=(
            jax.ShapeDtypeStruct((2, 256, 1024), F32),
            jax.ShapeDtypeStruct((2, 8, 1024), F32),
            jax.ShapeDtypeStruct((2, 8, 1024), F32),
        ),
        in_specs=[vmem, vmem, vmem],
        out_specs=(anyspec, anyspec, anyspec),
        scratch_shapes=[
            vm((CHUNKS, rows, 1024), F32),
            dma((CHUNKS,)),
            dma((4,)),
        ],
        compiler_params=pltpu.CompilerParams(vmem_limit_bytes=24 * 1024 * 1024),
        name="mix",
    )(w, h, r)
    return (
        mixed.reshape(1, 1, 2, 256, 1024),
        next_rx.reshape(1, 1, 2, 8, 1024),
        next_ry.reshape(1, 1, 2, 8, 1024),
    )


def solution(mesh):
    wide = P("rx", "ry", None, "tp", None)
    narrow = P("rx", "ry", None, None, None)
    return jax.shard_map(
        per_device, mesh=mesh, in_specs=(wide, narrow, narrow), out_specs=(wide, narrow, narrow), check_vma=False
    )
```

```python
import jax
import jax.numpy as jnp
from jax import lax
from jax.experimental import pallas as pl
from jax.experimental.pallas import tpu as pltpu
from jax.sharding import PartitionSpec as P

MESH = pl.DeviceIdType.MESH
F32 = jnp.float32
BF16 = jnp.bfloat16
NZ, NY = 8, 4
Z_ORDER = (4, 5, 3, 6, 2, 7, 1, 0)
NT = (((1,), (1,)), ((), ()))
NN = (((1,), (0,)), ((), ()))


def split3(x):
    hi = x.astype(BF16)
    rest = x - hi.astype(F32)
    mid = rest.astype(BF16)
    low = (rest - mid.astype(F32)).astype(BF16)
    return hi, mid, low


def dot6(x, wh, wm, wl, dims):
    rows = x.shape[0]
    hi, mid, low = split3(x)
    a = lax.dot_general(jnp.concatenate([hi, mid, low], 0), wh, dims, preferred_element_type=F32)
    b = lax.dot_general(jnp.concatenate([hi, mid], 0), wm, dims, preferred_element_type=F32)
    c = lax.dot_general(hi, wl, dims, preferred_element_type=F32)
    small = (c + b[rows:]) + a[2 * rows :]
    return a[:rows] + ((a[rows : 2 * rows] + b[:rows]) + small)


GATHER_ORDER = [(zz, yy) for zz in range(NZ) for yy in range(NY)]


def gossip(
    w_hbm, fx_hbm, fy_hbm, r_out, h_out,
    q, wv, wh, wm, wl, own, nb, p, c, inbox, g1, g2, g3, f,
    load_sem, fac_s, fac_r, own_s, own_r, sum_s, sum_r, all_s, all_r, g1_s, g1_r, g2_s, g2_r, g3_s, g3_r, heard,
):
    a, b, t = lax.axis_index("rx"), lax.axis_index("ry"), lax.axis_index("tp")
    z, y = lax.div(t, NY), lax.rem(t, NY)
    zs = [lax.rem(z + k, NZ) for k in range(NZ)]
    ys = [lax.rem(y + k, NY) for k in range(NY)]
    near = [(lax.rem(a + 3, 4), b), (a, lax.rem(b + 3, 4)), (lax.rem(a + 1, 4), b), (a, lax.rem(b + 1, 4))]
    near_dev = [(ra, rb, t) for ra, rb in near]

    def at(zz, yy):
        return (a, b, zz * NY + yy)

    beside = [at(zs[1], y), at(zs[7], y)]
    across = [at(z, ys[1]), at(z, ys[3])]
    barrier = pltpu.get_barrier_semaphore()
    for dev in near_dev + beside + across:
        pl.semaphore_signal(barrier, inc=1, device_id=dev, device_id_type=MESH)
    rounds = [across + beside, across + [at(zs[2], y), at(zs[6], y)], [at(zs[k], y) for k in Z_ORDER[:-1]]]

    def tell(i):
        for dev in rounds[i]:
            pl.semaphore_signal(heard.at[i], inc=1, device_id=dev, device_id_type=MESH)

    def hear(i):
        pl.semaphore_wait(heard.at[i], len(rounds[i]))

    def send(src, dst, ssem, rsem, dev):
        pltpu.make_async_remote_copy(
            src_ref=src, dst_ref=dst, send_sem=ssem, recv_sem=rsem, device_id=dev, device_id_type=MESH
        ).start()

    def counted(ref, sem):
        return pltpu.make_async_remote_copy(
            src_ref=ref, dst_ref=ref, send_sem=sem, recv_sem=sem, device_id=near_dev[0], device_id_type=MESH
        )

    loads = [
        pltpu.make_async_copy(fx_hbm, q.at[2], load_sem.at[0]),
        pltpu.make_async_copy(fy_hbm, q.at[3], load_sem.at[1]),
        pltpu.make_async_copy(w_hbm.at[0], wv.at[0], load_sem.at[2]),
        pltpu.make_async_copy(w_hbm.at[1], wv.at[1], load_sem.at[3]),
    ]
    for load in loads:
        load.start()

    turn = [2 * lax.rem(a, 2), 2 * lax.rem(a + b, 2)]
    owner = [lax.rem(slot + turn[slot % 2], NY) for slot in range(4)]
    from_owner = [lax.rem(y + NY - owner[slot], NY) for slot in range(4)]
    odd = lax.rem(y, 2)
    mine = lax.rem(y + (1 - odd) * turn[0] + odd * turn[1], NY)
    step = 3 - 2 * lax.div(mine, 2)
    far_a, far_b = lax.rem(a + (1 - odd) * step, 4), lax.rem(b + odd * step, 4)
    my_matrix = 1 - lax.div(mine, 2)
    my_tile = (mine * NZ + z) * 2 + my_matrix
    far_tile = (lax.rem(mine + 2, 4) * NZ + z) * 2 + my_matrix

    pl.semaphore_wait(barrier, 8)
    tell(0)
    for s in (2, 3):
        loads[s - 2].wait()
        send(q.at[s], q.at[s - 2], fac_s, fac_r, near_dev[s])

    def project(first):
        for m in range(2):
            x = q[pl.ds(first, 2), m].reshape(16, 1024)
            res = dot6(x, wh[m], wm[m], wl[m], NT)
            for i in range(2):
                own[first + i, m] = res[8 * i : 8 * i + 8]
        for s in (first, first + 1):
            send(own.at[s], nb.at[s ^ 2], own_s, own_r.at[1 - first // 2], near_dev[s])

    def differ(first):
        part = pl.ds(first, 2)
        counted(nb.at[part], own_r.at[first // 2]).wait_recv()
        p[part] = own[part] - nb[part]

    def back(first, m):
        x = p[pl.ds(first, 2), m].reshape(16, 256)
        res = dot6(x, wh[m], wm[m], wl[m], NN)
        for i in range(2):
            for j in range(NZ):
                c[((first + i) * NZ + j) * 2 + m] = res[8 * i : 8 * i + 8, 128 * j : 128 * j + 128]

    def share(first, m, order):
        here = m == 1 - first // 2
        for k in order:
            for s in (first, first + 1):
                src = c.at[(s * NZ + zs[k]) * 2 + m]
                dst = inbox.at[((NZ - k) % NZ) * NY + from_owner[s] + (0 if here else 32)]
                ra, rb = (a, b) if here else near[s]
                dev = (ra, rb, zs[k] * NY + owner[s])
                if here and k == 0:

                    @pl.when(owner[s] != y)
                    def _():
                        send(src, dst, sum_s, sum_r, dev)
                else:
                    send(src, dst, sum_s, sum_r, dev)

    for m in range(2):
        loads[2 + m].wait()
        hi, mid, low = split3(wv[m])
        wh[m], wm[m], wl[m] = hi, mid, low
    project(2)
    hear(0)
    tell(1)
    counted(q.at[pl.ds(0, 2)], fac_r).wait_recv()
    hear(1)
    tell(2)
    project(0)
    differ(0)

    rows = p[0:2].reshape(32, 256)
    gram = lax.dot_general(
        rows, jnp.concatenate([rows] * 4, 0), NT, precision=lax.Precision.HIGHEST, preferred_element_type=F32
    )
    lane = lax.broadcasted_iota(jnp.int32, (8, 128), 1)
    block = (lane // 8) % 4
    tile = jnp.zeros((8, 128), F32)
    for i in range(4):
        tile = tile + jnp.where(block == i, gram[8 * i : 8 * i + 8], 0.0)
    g1[y] = tile
    for k in (2, 1, 3):
        send(g1.at[y], g1.at[y], g1_s, g1_r, at(z, ys[k]))
    for m in range(2):
        back(0, m)
    hear(2)
    for k in Z_ORDER[:4]:
        for m in range(2):
            share(0, m, (k,))
    differ(2)
    for m in range(2):
        back(2, m)
    for k in Z_ORDER[:4]:
        for m in range(2):
            share(2, m, (k,))
    for k in Z_ORDER[4:6]:
        for m in range(2):
            share(0, m, (k,))
            share(2, m, (k,))

    counted(g1.at[pl.ds(0, NY - 1)], g1_r).wait_recv()
    g2[z] = (g1[0] + g1[1]) + (g1[2] + g1[3])
    for k in Z_ORDER[:-1]:
        send(g2.at[z], g2.at[z], g2_s, g2_r, at(zs[k], y))
    for k in Z_ORDER[6:]:
        for m in range(2):
            share(0, m, (k,))
            share(2, m, (k,))
    counted(g2.at[pl.ds(0, NZ - 1)], g2_r).wait_recv()
    g3[2] = ((g2[0] + g2[1]) + (g2[2] + g2[3])) + ((g2[4] + g2[5]) + (g2[6] + g2[7]))
    for s in (0, 1):
        send(g3.at[2], g3.at[s], g3_s, g3_r, near_dev[s])

    counted(inbox.at[pl.ds(1, 63)], sum_r).wait_recv()
    parts = [c[my_tile], inbox[1], inbox[2], inbox[3]]
    for i in range(4, 64):
        parts[i % 4] = parts[i % 4] + inbox[i]
    f[my_tile] = (parts[0] + parts[1]) + (parts[2] + parts[3])
    for zz, yy in GATHER_ORDER:
        there = zz * NY + yy
        send(f.at[my_tile], f.at[far_tile], all_s, all_r, (far_a, far_b, there))

        @pl.when(t != there)
        def _():
            send(f.at[my_tile], f.at[my_tile], all_s, all_r, (a, b, there))

    counted(g3.at[pl.ds(0, 2)], g3_r).wait_recv()
    tile = jnp.where(lane < 32, g3[2], jnp.where(lane < 48, g3[0], g3[1]))
    row = lax.broadcasted_iota(jnp.int32, (8, 128), 0)
    cols = [tile] + [pltpu.roll(tile, 128 - j, 1) for j in range(1, 8)]
    lower, inverse_diag = [], []
    for k in range(8):
        pivot = jnp.broadcast_to(cols[k][k : k + 1], (8, 128))
        inv = 1.0 / jnp.sqrt(pivot)
        col = cols[k] * inv
        lower.append(jnp.where(row > k, col, 0.0))
        inverse_diag.append(inv)
        for j in range(k + 1, 8):
            cols[j] = cols[j] - col * jnp.broadcast_to(col[j : j + 1], (8, 128))
    inv_cols = [jnp.where(row == j, 1.0, 0.0).astype(F32) for j in range(8)]
    for k in range(8):
        for j in range(k + 1):
            cur = inv_cols[j]
            pivot_row = jnp.broadcast_to(cur[k : k + 1], (8, 128)) * inverse_diag[k]
            cur = cur - lower[k] * pivot_row
            inv_cols[j] = jnp.where(row == k, pivot_row, cur)

    def solve(i, x):
        total = inv_cols[0][:, 8 * i : 8 * i + 1] * x[0:1]
        for j in range(1, 8):
            total = total + inv_cols[j][:, 8 * i : 8 * i + 1] * x[j : j + 1]
        return total

    for m in range(2):
        for s in range(4):
            h_out[m, s] = solve(2 * s + m, p[s, m])

    counted(f.at[pl.ds(0, 63)], all_r).wait_recv()
    for m in range(2):
        for s in range(4):
            r_out[m, s] = solve(2 * s + m, jnp.concatenate([f[(s * NZ + j) * 2 + m] for j in range(NZ)], 1))

    counted(q.at[pl.ds(2, 2)], fac_s).wait_send()
    counted(own, own_s).wait_send()
    counted(c.at[pl.ds(0, 63)], sum_s).wait_send()
    counted(f.at[pl.ds(0, 63)], all_s).wait_send()
    counted(g1.at[pl.ds(0, NY - 1)], g1_s).wait_send()
    counted(g2.at[pl.ds(0, NZ - 1)], g2_s).wait_send()
    counted(g3.at[pl.ds(0, 2)], g3_s).wait_send()


COLUMNS = 256


def mix(w_ref, h_ref, r_ref, out_hbm, nx_hbm, ny_hbm, ov, out_sem, small_sem):
    stores = []
    for m in range(2):
        stores.append(pltpu.make_async_copy(r_ref.at[m, 2], nx_hbm.at[m], small_sem.at[m]))
        stores.append(pltpu.make_async_copy(r_ref.at[m, 3], ny_hbm.at[m], small_sem.at[2 + m]))
    for store in stores:
        store.start()
    for m in range(2):
        hh, hl, _ = split3(h_ref[m].reshape(32, 256))
        left = jnp.concatenate([hh, hh, hl], 0)
        for i in range(1024 // COLUMNS):
            part = pl.ds(i * COLUMNS, COLUMNS)
            rh, rl, _ = split3(r_ref[m, :, :, part].reshape(32, COLUMNS))
            right = jnp.concatenate([rh, rl, rh], 0)
            term = lax.dot_general(left, right, (((0,), (0,)), ((), ())), preferred_element_type=F32)
            n = m * (1024 // COLUMNS) + i
            ov[n] = w_ref[m, :, part] - 0.2 * term
            store = pltpu.make_async_copy(ov.at[n], out_hbm.at[m, :, part], out_sem.at[n])
            store.start()
            stores.append(store)
    for store in stores:
        store.wait()


def per_device(weights, factors_rx, factors_ry):
    w = weights.reshape(2, 256, 1024)
    vm = pltpu.VMEM
    dma = pltpu.SemaphoreType.DMA
    anyspec = pl.BlockSpec(memory_space=pl.ANY)
    hbm = pl.BlockSpec(memory_space=pltpu.HBM)
    vmem = pl.BlockSpec(memory_space=pltpu.VMEM)
    tile = (8, 128)
    r, h = pl.pallas_call(
        gossip,
        out_shape=(
            jax.ShapeDtypeStruct((2, 4, 8, 1024), F32),
            jax.ShapeDtypeStruct((2, 4, 8, 256), F32),
        ),
        in_specs=[hbm] * 3,
        out_specs=(vmem, vmem),
        scratch_shapes=[
            vm((4, 2, 8, 1024), F32),
            vm((2, 256, 1024), F32),
            vm((2, 256, 1024), BF16),
            vm((2, 256, 1024), BF16),
            vm((2, 256, 1024), BF16),
            vm((4, 2, 8, 256), F32),
            vm((4, 2, 8, 256), F32),
            vm((4, 2, 8, 256), F32),
            vm((64, *tile), F32),
            vm((64, *tile), F32),
            vm((NY, *tile), F32),
            vm((NZ, *tile), F32),
            vm((3, *tile), F32),
            vm((64, *tile), F32),
            dma((4,)),
            dma, dma,
            dma, dma((2,)),
            dma, dma,
            dma, dma,
            dma, dma,
            dma, dma,
            dma, dma,
            pltpu.SemaphoreType.REGULAR((3,)),
        ],
        compiler_params=pltpu.CompilerParams(
            collective_id=0, has_side_effects=True, vmem_limit_bytes=24 * 1024 * 1024
        ),
        name="gossip",
    )(*[pltpu.with_memory_space_constraint(x, pltpu.HBM) for x in (w, factors_rx.reshape(2, 8, 1024), factors_ry.reshape(2, 8, 1024))])
    mixed, next_rx, next_ry = pl.pallas_call(
        mix,
        out_shape=(
            jax.ShapeDtypeStruct((2, 256, 1024), F32),
            jax.ShapeDtypeStruct((2, 8, 1024), F32),
            jax.ShapeDtypeStruct((2, 8, 1024), F32),
        ),
        in_specs=[vmem, vmem, vmem],
        out_specs=(anyspec, anyspec, anyspec),
        scratch_shapes=[
            vm((2048 // COLUMNS, 256, COLUMNS), F32),
            dma((2048 // COLUMNS,)),
            dma((4,)),
        ],
        compiler_params=pltpu.CompilerParams(vmem_limit_bytes=24 * 1024 * 1024),
        name="mix",
    )(w, h, r)
    return (
        mixed.reshape(1, 1, 2, 256, 1024),
        next_rx.reshape(1, 1, 2, 8, 1024),
        next_ry.reshape(1, 1, 2, 8, 1024),
    )


def solution(mesh):
    wide = P("rx", "ry", None, "tp", None)
    narrow = P("rx", "ry", None, None, None)
    return jax.shard_map(
        per_device, mesh=mesh, in_specs=(wide, narrow, narrow), out_specs=(wide, narrow, narrow), check_vma=False
    )
```

```python
import jax
import jax.numpy as jnp
from jax import lax
from jax.experimental import pallas as pl
from jax.experimental.pallas import tpu as pltpu
from jax.sharding import PartitionSpec as P

MESH = pl.DeviceIdType.MESH
F32 = jnp.float32
BF16 = jnp.bfloat16
NZ, NY = 8, 4
Z_ORDER = (4, 5, 3, 6, 2, 7, 1, 0)
NT = (((1,), (1,)), ((), ()))
NN = (((1,), (0,)), ((), ()))


def split3(x):
    hi = x.astype(BF16)
    rest = x - hi.astype(F32)
    mid = rest.astype(BF16)
    low = (rest - mid.astype(F32)).astype(BF16)
    return hi, mid, low


def dot6(x, wh, wm, wl, dims):
    rows = x.shape[0]
    hi, mid, low = split3(x)
    a = lax.dot_general(jnp.concatenate([hi, mid, low], 0), wh, dims, preferred_element_type=F32)
    b = lax.dot_general(jnp.concatenate([hi, mid], 0), wm, dims, preferred_element_type=F32)
    c = lax.dot_general(hi, wl, dims, preferred_element_type=F32)
    small = (c + b[rows:]) + a[2 * rows :]
    return a[:rows] + ((a[rows : 2 * rows] + b[:rows]) + small)


GATHER_ORDER = [(zz, yy) for zz in range(NZ) for yy in range(NY)]


def gossip(
    w_hbm, fx_hbm, fy_hbm, r_out, h_out,
    q, wv, wh, wm, wl, th, tm, tl, own, nb, p, c, inbox, g1, g2, g3, f,
    load_sem, fac_s, fac_r, own_s, own_r, sum_s, sum_r, all_s, all_r, g1_s, g1_r, g2_s, g2_r, g3_s, g3_r, heard,
):
    a, b, t = lax.axis_index("rx"), lax.axis_index("ry"), lax.axis_index("tp")
    z, y = lax.div(t, NY), lax.rem(t, NY)
    zs = [lax.rem(z + k, NZ) for k in range(NZ)]
    ys = [lax.rem(y + k, NY) for k in range(NY)]
    near = [(lax.rem(a + 3, 4), b), (a, lax.rem(b + 3, 4)), (lax.rem(a + 1, 4), b), (a, lax.rem(b + 1, 4))]
    near_dev = [(ra, rb, t) for ra, rb in near]

    def at(zz, yy):
        return (a, b, zz * NY + yy)

    beside = [at(zs[1], y), at(zs[7], y)]
    across = [at(z, ys[1]), at(z, ys[3])]
    barrier = pltpu.get_barrier_semaphore()
    for dev in near_dev + beside + across:
        pl.semaphore_signal(barrier, inc=1, device_id=dev, device_id_type=MESH)
    rounds = [across + beside, across + [at(zs[2], y), at(zs[6], y)], [at(zs[k], y) for k in Z_ORDER[:-1]]]

    def tell(i):
        for dev in rounds[i]:
            pl.semaphore_signal(heard.at[i], inc=1, device_id=dev, device_id_type=MESH)

    def hear(i):
        pl.semaphore_wait(heard.at[i], len(rounds[i]))

    def send(src, dst, ssem, rsem, dev):
        pltpu.make_async_remote_copy(
            src_ref=src, dst_ref=dst, send_sem=ssem, recv_sem=rsem, device_id=dev, device_id_type=MESH
        ).start()

    def counted(ref, sem):
        return pltpu.make_async_remote_copy(
            src_ref=ref, dst_ref=ref, send_sem=sem, recv_sem=sem, device_id=near_dev[0], device_id_type=MESH
        )

    loads = [
        pltpu.make_async_copy(fx_hbm, q.at[2], load_sem.at[0]),
        pltpu.make_async_copy(fy_hbm, q.at[3], load_sem.at[1]),
        pltpu.make_async_copy(w_hbm.at[0], wv.at[0], load_sem.at[2]),
        pltpu.make_async_copy(w_hbm.at[1], wv.at[1], load_sem.at[3]),
    ]
    for load in loads:
        load.start()

    turn = [2 * lax.rem(a, 2), 2 * lax.rem(a + b, 2)]
    owner = [lax.rem(slot + turn[slot % 2], NY) for slot in range(4)]
    from_owner = [lax.rem(y + NY - owner[slot], NY) for slot in range(4)]
    odd = lax.rem(y, 2)
    mine = lax.rem(y + (1 - odd) * turn[0] + odd * turn[1], NY)
    step = 3 - 2 * lax.div(mine, 2)
    far_a, far_b = lax.rem(a + (1 - odd) * step, 4), lax.rem(b + odd * step, 4)
    my_matrix = 1 - lax.div(mine, 2)
    my_tile = (mine * NZ + z) * 2 + my_matrix
    far_tile = (lax.rem(mine + 2, 4) * NZ + z) * 2 + my_matrix

    pl.semaphore_wait(barrier, 8)
    tell(0)
    for s in (2, 3):
        loads[s - 2].wait()
        send(q.at[s], q.at[s - 2], fac_s, fac_r, near_dev[s])

    def project(first):
        for m in range(2):
            x = q[pl.ds(first, 2), m].reshape(16, 1024)
            if first == 2:
                res = dot6(x, wh[m], wm[m], wl[m], NT)
            else:
                res = dot6(x, th[m], tm[m], tl[m], NN)
            for i in range(2):
                own[first + i, m] = res[8 * i : 8 * i + 8]
        for s in (first, first + 1):
            send(own.at[s], nb.at[s ^ 2], own_s, own_r.at[1 - first // 2], near_dev[s])

    def differ(first):
        part = pl.ds(first, 2)
        counted(nb.at[part], own_r.at[first // 2]).wait_recv()
        p[part] = own[part] - nb[part]

    def back(first, m):
        x = p[pl.ds(first, 2), m].reshape(16, 256)
        res = dot6(x, wh[m], wm[m], wl[m], NN)
        for i in range(2):
            for j in range(NZ):
                c[((first + i) * NZ + j) * 2 + m] = res[8 * i : 8 * i + 8, 128 * j : 128 * j + 128]

    def share(first, m, order):
        here = m == 1 - first // 2
        for k in order:
            for s in (first, first + 1):
                src = c.at[(s * NZ + zs[k]) * 2 + m]
                dst = inbox.at[((NZ - k) % NZ) * NY + from_owner[s] + (0 if here else 32)]
                ra, rb = (a, b) if here else near[s]
                dev = (ra, rb, zs[k] * NY + owner[s])
                if here and k == 0:

                    @pl.when(owner[s] != y)
                    def _():
                        send(src, dst, sum_s, sum_r, dev)
                else:
                    send(src, dst, sum_s, sum_r, dev)

    for m in range(2):
        loads[2 + m].wait()
        hi, mid, low = split3(wv[m])
        wh[m], wm[m], wl[m] = hi, mid, low
    project(2)
    hear(0)
    tell(1)
    for m in range(2):
        th[m], tm[m], tl[m] = wh[m].T, wm[m].T, wl[m].T
    hear(1)
    tell(2)
    counted(q.at[pl.ds(0, 2)], fac_r).wait_recv()
    project(0)
    differ(0)

    rows = p[0:2].reshape(32, 256)
    gram = lax.dot_general(
        rows, jnp.concatenate([rows] * 4, 0), NT, precision=lax.Precision.HIGHEST, preferred_element_type=F32
    )
    lane = lax.broadcasted_iota(jnp.int32, (8, 128), 1)
    block = (lane // 8) % 4
    tile = jnp.zeros((8, 128), F32)
    for i in range(4):
        tile = tile + jnp.where(block == i, gram[8 * i : 8 * i + 8], 0.0)
    g1[y] = tile
    for k in (2, 1, 3):
        send(g1.at[y], g1.at[y], g1_s, g1_r, at(z, ys[k]))
    for m in range(2):
        back(0, m)
    hear(2)
    for k in Z_ORDER[:4]:
        for m in range(2):
            share(0, m, (k,))
    differ(2)
    for m in range(2):
        back(2, m)
    for k in Z_ORDER[:4]:
        for m in range(2):
            share(2, m, (k,))
    for k in Z_ORDER[4:6]:
        for m in range(2):
            share(0, m, (k,))
            share(2, m, (k,))

    counted(g1.at[pl.ds(0, NY - 1)], g1_r).wait_recv()
    g2[z] = (g1[0] + g1[1]) + (g1[2] + g1[3])
    for k in Z_ORDER[:-1]:
        send(g2.at[z], g2.at[z], g2_s, g2_r, at(zs[k], y))
    for k in Z_ORDER[6:]:
        for m in range(2):
            share(0, m, (k,))
            share(2, m, (k,))
    counted(g2.at[pl.ds(0, NZ - 1)], g2_r).wait_recv()
    g3[2] = ((g2[0] + g2[1]) + (g2[2] + g2[3])) + ((g2[4] + g2[5]) + (g2[6] + g2[7]))
    for s in (0, 1):
        send(g3.at[2], g3.at[s], g3_s, g3_r, near_dev[s])

    counted(inbox.at[pl.ds(1, 63)], sum_r).wait_recv()
    parts = [c[my_tile], inbox[1], inbox[2], inbox[3]]
    for i in range(4, 64):
        parts[i % 4] = parts[i % 4] + inbox[i]
    f[my_tile] = (parts[0] + parts[1]) + (parts[2] + parts[3])
    for zz, yy in GATHER_ORDER:
        there = zz * NY + yy
        send(f.at[my_tile], f.at[far_tile], all_s, all_r, (far_a, far_b, there))

        @pl.when(t != there)
        def _():
            send(f.at[my_tile], f.at[my_tile], all_s, all_r, (a, b, there))

    counted(g3.at[pl.ds(0, 2)], g3_r).wait_recv()
    tile = jnp.where(lane < 32, g3[2], jnp.where(lane < 48, g3[0], g3[1]))
    row = lax.broadcasted_iota(jnp.int32, (8, 128), 0)
    cols = [tile] + [pltpu.roll(tile, 128 - j, 1) for j in range(1, 8)]
    lower, inverse_diag = [], []
    for k in range(8):
        pivot = jnp.broadcast_to(cols[k][k : k + 1], (8, 128))
        inv = 1.0 / jnp.sqrt(pivot)
        col = cols[k] * inv
        lower.append(jnp.where(row > k, col, 0.0))
        inverse_diag.append(inv)
        for j in range(k + 1, 8):
            cols[j] = cols[j] - col * jnp.broadcast_to(col[j : j + 1], (8, 128))
    inv_cols = [jnp.where(row == j, 1.0, 0.0).astype(F32) for j in range(8)]
    for k in range(8):
        for j in range(k + 1):
            cur = inv_cols[j]
            pivot_row = jnp.broadcast_to(cur[k : k + 1], (8, 128)) * inverse_diag[k]
            cur = cur - lower[k] * pivot_row
            inv_cols[j] = jnp.where(row == k, pivot_row, cur)

    def solve(i, x):
        total = inv_cols[0][:, 8 * i : 8 * i + 1] * x[0:1]
        for j in range(1, 8):
            total = total + inv_cols[j][:, 8 * i : 8 * i + 1] * x[j : j + 1]
        return total

    for m in range(2):
        for s in range(4):
            h_out[m, s] = solve(2 * s + m, p[s, m])

    counted(f.at[pl.ds(0, 63)], all_r).wait_recv()
    for m in range(2):
        for s in range(4):
            r_out[m, s] = solve(2 * s + m, jnp.concatenate([f[(s * NZ + j) * 2 + m] for j in range(NZ)], 1))

    counted(q.at[pl.ds(2, 2)], fac_s).wait_send()
    counted(own, own_s).wait_send()
    counted(c.at[pl.ds(0, 63)], sum_s).wait_send()
    counted(f.at[pl.ds(0, 63)], all_s).wait_send()
    counted(g1.at[pl.ds(0, NY - 1)], g1_s).wait_send()
    counted(g2.at[pl.ds(0, NZ - 1)], g2_s).wait_send()
    counted(g3.at[pl.ds(0, 2)], g3_s).wait_send()


COLUMNS = 256


def mix(w_ref, h_ref, r_ref, out_hbm, nx_hbm, ny_hbm, ov, out_sem, small_sem):
    stores = []
    for m in range(2):
        stores.append(pltpu.make_async_copy(r_ref.at[m, 2], nx_hbm.at[m], small_sem.at[m]))
        stores.append(pltpu.make_async_copy(r_ref.at[m, 3], ny_hbm.at[m], small_sem.at[2 + m]))
    for store in stores:
        store.start()
    for m in range(2):
        hh, hl, _ = split3(h_ref[m].reshape(32, 256))
        left = jnp.concatenate([hh, hh, hl], 0)
        for i in range(1024 // COLUMNS):
            part = pl.ds(i * COLUMNS, COLUMNS)
            rh, rl, _ = split3(r_ref[m, :, :, part].reshape(32, COLUMNS))
            right = jnp.concatenate([rh, rl, rh], 0)
            term = lax.dot_general(left, right, (((0,), (0,)), ((), ())), preferred_element_type=F32)
            n = m * (1024 // COLUMNS) + i
            ov[n] = w_ref[m, :, part] - 0.2 * term
            store = pltpu.make_async_copy(ov.at[n], out_hbm.at[m, :, part], out_sem.at[n])
            store.start()
            stores.append(store)
    for store in stores:
        store.wait()


def per_device(weights, factors_rx, factors_ry):
    w = weights.reshape(2, 256, 1024)
    vm = pltpu.VMEM
    dma = pltpu.SemaphoreType.DMA
    anyspec = pl.BlockSpec(memory_space=pl.ANY)
    hbm = pl.BlockSpec(memory_space=pltpu.HBM)
    vmem = pl.BlockSpec(memory_space=pltpu.VMEM)
    tile = (8, 128)
    r, h = pl.pallas_call(
        gossip,
        out_shape=(
            jax.ShapeDtypeStruct((2, 4, 8, 1024), F32),
            jax.ShapeDtypeStruct((2, 4, 8, 256), F32),
        ),
        in_specs=[hbm] * 3,
        out_specs=(vmem, vmem),
        scratch_shapes=[
            vm((4, 2, 8, 1024), F32),
            vm((2, 256, 1024), F32),
            vm((2, 256, 1024), BF16),
            vm((2, 256, 1024), BF16),
            vm((2, 256, 1024), BF16),
            vm((2, 1024, 256), BF16),
            vm((2, 1024, 256), BF16),
            vm((2, 1024, 256), BF16),
            vm((4, 2, 8, 256), F32),
            vm((4, 2, 8, 256), F32),
            vm((4, 2, 8, 256), F32),
            vm((64, *tile), F32),
            vm((64, *tile), F32),
            vm((NY, *tile), F32),
            vm((NZ, *tile), F32),
            vm((3, *tile), F32),
            vm((64, *tile), F32),
            dma((4,)),
            dma, dma,
            dma, dma((2,)),
            dma, dma,
            dma, dma,
            dma, dma,
            dma, dma,
            dma, dma,
            pltpu.SemaphoreType.REGULAR((3,)),
        ],
        compiler_params=pltpu.CompilerParams(
            collective_id=0, has_side_effects=True, vmem_limit_bytes=24 * 1024 * 1024
        ),
        name="gossip",
    )(*[pltpu.with_memory_space_constraint(x, pltpu.HBM) for x in (w, factors_rx.reshape(2, 8, 1024), factors_ry.reshape(2, 8, 1024))])
    mixed, next_rx, next_ry = pl.pallas_call(
        mix,
        out_shape=(
            jax.ShapeDtypeStruct((2, 256, 1024), F32),
            jax.ShapeDtypeStruct((2, 8, 1024), F32),
            jax.ShapeDtypeStruct((2, 8, 1024), F32),
        ),
        in_specs=[vmem, vmem, vmem],
        out_specs=(anyspec, anyspec, anyspec),
        scratch_shapes=[
            vm((2048 // COLUMNS, 256, COLUMNS), F32),
            dma((2048 // COLUMNS,)),
            dma((4,)),
        ],
        compiler_params=pltpu.CompilerParams(vmem_limit_bytes=24 * 1024 * 1024),
        name="mix",
    )(w, h, r)
    return (
        mixed.reshape(1, 1, 2, 256, 1024),
        next_rx.reshape(1, 1, 2, 8, 1024),
        next_ry.reshape(1, 1, 2, 8, 1024),
    )


def solution(mesh):
    wide = P("rx", "ry", None, "tp", None)
    narrow = P("rx", "ry", None, None, None)
    return jax.shard_map(
        per_device, mesh=mesh, in_specs=(wide, narrow, narrow), out_specs=(wide, narrow, narrow), check_vma=False
    )
```

```python
import jax
import jax.numpy as jnp
from jax import lax
from jax.experimental import pallas as pl
from jax.experimental.pallas import tpu as pltpu
from jax.sharding import PartitionSpec as P

MESH = pl.DeviceIdType.MESH
F32 = jnp.float32
BF16 = jnp.bfloat16
NZ, NY = 8, 4
Z_ORDER = (4, 5, 3, 6, 2, 7, 1, 0)
NT = (((1,), (1,)), ((), ()))
NN = (((1,), (0,)), ((), ()))


def split3(x):
    hi = x.astype(BF16)
    rest = x - hi.astype(F32)
    mid = rest.astype(BF16)
    low = (rest - mid.astype(F32)).astype(BF16)
    return hi, mid, low


def dot6(x, wh, wm, wl, dims):
    rows = x.shape[0]
    hi, mid, low = split3(x)
    a = lax.dot_general(jnp.concatenate([hi, mid, low], 0), wh, dims, preferred_element_type=F32)
    b = lax.dot_general(jnp.concatenate([hi, mid], 0), wm, dims, preferred_element_type=F32)
    c = lax.dot_general(hi, wl, dims, preferred_element_type=F32)
    small = (c + b[rows:]) + a[2 * rows :]
    return a[:rows] + ((a[rows : 2 * rows] + b[:rows]) + small)


GATHER_ORDER = [(zz, j) for zz in range(NZ) for j in (2, 1, 3, 0)]


def gossip(
    w_hbm, fx_hbm, fy_hbm, r_out, h_out,
    q, wv, wh, wm, wl, th, tm, tl, own, nb, p, c, inbox, g1, g2, g3, f,
    load_sem, fac_s, fac_r, own_s, own_r, sum_s, sum_r, all_s, all_r, g1_s, g1_r, g2_s, g2_r, g3_s, g3_r, heard,
):
    a, b, t = lax.axis_index("rx"), lax.axis_index("ry"), lax.axis_index("tp")
    z, y = lax.div(t, NY), lax.rem(t, NY)
    zs = [lax.rem(z + k, NZ) for k in range(NZ)]
    ys = [lax.rem(y + k, NY) for k in range(NY)]
    near = [(lax.rem(a + 3, 4), b), (a, lax.rem(b + 3, 4)), (lax.rem(a + 1, 4), b), (a, lax.rem(b + 1, 4))]
    near_dev = [(ra, rb, t) for ra, rb in near]

    def at(zz, yy):
        return (a, b, zz * NY + yy)

    beside = [at(zs[1], y), at(zs[7], y)]
    across = [at(z, ys[1]), at(z, ys[3])]
    barrier = pltpu.get_barrier_semaphore()
    for dev in near_dev + beside + across:
        pl.semaphore_signal(barrier, inc=1, device_id=dev, device_id_type=MESH)
    rounds = [across + beside, across + [at(zs[2], y), at(zs[6], y)], [at(zs[k], y) for k in Z_ORDER[:-1]]]

    def tell(i):
        for dev in rounds[i]:
            pl.semaphore_signal(heard.at[i], inc=1, device_id=dev, device_id_type=MESH)

    def hear(i):
        pl.semaphore_wait(heard.at[i], len(rounds[i]))

    def send(src, dst, ssem, rsem, dev):
        pltpu.make_async_remote_copy(
            src_ref=src, dst_ref=dst, send_sem=ssem, recv_sem=rsem, device_id=dev, device_id_type=MESH
        ).start()

    def counted(ref, sem):
        return pltpu.make_async_remote_copy(
            src_ref=ref, dst_ref=ref, send_sem=sem, recv_sem=sem, device_id=near_dev[0], device_id_type=MESH
        )

    loads = [
        pltpu.make_async_copy(fx_hbm, q.at[2], load_sem.at[0]),
        pltpu.make_async_copy(fy_hbm, q.at[3], load_sem.at[1]),
        pltpu.make_async_copy(w_hbm.at[0], wv.at[0], load_sem.at[2]),
        pltpu.make_async_copy(w_hbm.at[1], wv.at[1], load_sem.at[3]),
    ]
    for load in loads:
        load.start()

    turn = [2 * lax.rem(a, 2), 2 * lax.rem(a + b, 2)]
    owner = [lax.rem(slot + turn[slot % 2], NY) for slot in range(4)]
    from_owner = [lax.rem(y + NY - owner[slot], NY) for slot in range(4)]
    odd = lax.rem(y, 2)
    mine = lax.rem(y + (1 - odd) * turn[0] + odd * turn[1], NY)
    step = 3 - 2 * lax.div(mine, 2)
    far_a, far_b = lax.rem(a + (1 - odd) * step, 4), lax.rem(b + odd * step, 4)
    my_matrix = 1 - lax.div(mine, 2)
    my_tile = (mine * NZ + z) * 2 + my_matrix
    far_tile = (lax.rem(mine + 2, 4) * NZ + z) * 2 + my_matrix

    pl.semaphore_wait(barrier, 8)
    tell(0)
    for s in (2, 3):
        loads[s - 2].wait()
        send(q.at[s], q.at[s - 2], fac_s, fac_r, near_dev[s])

    def project(first):
        for m in range(2):
            x = q[pl.ds(first, 2), m].reshape(16, 1024)
            if first == 2:
                res = dot6(x, wh[m], wm[m], wl[m], NT)
            else:
                res = dot6(x, th[m], tm[m], tl[m], NN)
            for i in range(2):
                own[first + i, m] = res[8 * i : 8 * i + 8]
        for s in (first, first + 1):
            send(own.at[s], nb.at[s ^ 2], own_s, own_r.at[1 - first // 2], near_dev[s])

    def differ(first):
        part = pl.ds(first, 2)
        counted(nb.at[part], own_r.at[first // 2]).wait_recv()
        p[part] = own[part] - nb[part]

    def back(first, m):
        x = p[pl.ds(first, 2), m].reshape(16, 256)
        res = dot6(x, wh[m], wm[m], wl[m], NN)
        for i in range(2):
            for j in range(NZ):
                c[((first + i) * NZ + j) * 2 + m] = res[8 * i : 8 * i + 8, 128 * j : 128 * j + 128]

    def share(first, m, order):
        here = m == 1 - first // 2
        for k in order:
            for s in (first, first + 1):
                src = c.at[(s * NZ + zs[k]) * 2 + m]
                dst = inbox.at[((NZ - k) % NZ) * NY + from_owner[s] + (0 if here else 32)]
                ra, rb = (a, b) if here else near[s]
                dev = (ra, rb, zs[k] * NY + owner[s])
                if here and k == 0:

                    @pl.when(owner[s] != y)
                    def _():
                        send(src, dst, sum_s, sum_r, dev)
                else:
                    send(src, dst, sum_s, sum_r, dev)

    for m in range(2):
        loads[2 + m].wait()
        hi, mid, low = split3(wv[m])
        wh[m], wm[m], wl[m] = hi, mid, low
    project(2)
    hear(0)
    tell(1)
    for m in range(2):
        th[m], tm[m], tl[m] = wh[m].T, wm[m].T, wl[m].T
    hear(1)
    tell(2)
    counted(q.at[pl.ds(0, 2)], fac_r).wait_recv()
    project(0)
    differ(0)

    rows = p[0:2].reshape(32, 256)
    gram = lax.dot_general(
        rows, jnp.concatenate([rows] * 4, 0), NT, precision=lax.Precision.HIGHEST, preferred_element_type=F32
    )
    lane = lax.broadcasted_iota(jnp.int32, (8, 128), 1)
    block = (lane // 8) % 4
    tile = jnp.zeros((8, 128), F32)
    for i in range(4):
        tile = tile + jnp.where(block == i, gram[8 * i : 8 * i + 8], 0.0)
    g1[y] = tile
    for k in (2, 1, 3):
        send(g1.at[y], g1.at[y], g1_s, g1_r, at(z, ys[k]))
    for m in range(2):
        back(0, m)
    hear(2)
    for k in Z_ORDER[:4]:
        for m in range(2):
            share(0, m, (k,))
    differ(2)
    for m in range(2):
        back(2, m)
    for k in Z_ORDER[:4]:
        for m in range(2):
            share(2, m, (k,))
    for k in Z_ORDER[4:6]:
        for m in range(2):
            share(0, m, (k,))
            share(2, m, (k,))

    counted(g1.at[pl.ds(0, NY - 1)], g1_r).wait_recv()
    g2[z] = (g1[0] + g1[1]) + (g1[2] + g1[3])
    for k in Z_ORDER[:-1]:
        send(g2.at[z], g2.at[z], g2_s, g2_r, at(zs[k], y))
    for k in Z_ORDER[6:]:
        for m in range(2):
            share(0, m, (k,))
            share(2, m, (k,))
    counted(g2.at[pl.ds(0, NZ - 1)], g2_r).wait_recv()
    g3[2] = ((g2[0] + g2[1]) + (g2[2] + g2[3])) + ((g2[4] + g2[5]) + (g2[6] + g2[7]))
    for s in (0, 1):
        send(g3.at[2], g3.at[s], g3_s, g3_r, near_dev[s])

    counted(inbox.at[pl.ds(1, 63)], sum_r).wait_recv()
    parts = [c[my_tile], inbox[1], inbox[2], inbox[3]]
    for i in range(4, 64):
        parts[i % 4] = parts[i % 4] + inbox[i]
    f[my_tile] = (parts[0] + parts[1]) + (parts[2] + parts[3])
    for zz, j in GATHER_ORDER:
        there = zz * NY + ys[j]
        send(f.at[my_tile], f.at[far_tile], all_s, all_r, (far_a, far_b, there))
        if j:
            send(f.at[my_tile], f.at[my_tile], all_s, all_r, (a, b, there))
        else:

            @pl.when(z != zz)
            def _():
                send(f.at[my_tile], f.at[my_tile], all_s, all_r, (a, b, there))

    counted(g3.at[pl.ds(0, 2)], g3_r).wait_recv()
    tile = jnp.where(lane < 32, g3[2], jnp.where(lane < 48, g3[0], g3[1]))
    row = lax.broadcasted_iota(jnp.int32, (8, 128), 0)
    cols = [tile] + [pltpu.roll(tile, 128 - j, 1) for j in range(1, 8)]
    lower, inverse_diag = [], []
    for k in range(8):
        pivot = jnp.broadcast_to(cols[k][k : k + 1], (8, 128))
        inv = 1.0 / jnp.sqrt(pivot)
        col = cols[k] * inv
        lower.append(jnp.where(row > k, col, 0.0))
        inverse_diag.append(inv)
        for j in range(k + 1, 8):
            cols[j] = cols[j] - col * jnp.broadcast_to(col[j : j + 1], (8, 128))
    inv_cols = [jnp.where(row == j, 1.0, 0.0).astype(F32) for j in range(8)]
    for k in range(8):
        for j in range(k + 1):
            cur = inv_cols[j]
            pivot_row = jnp.broadcast_to(cur[k : k + 1], (8, 128)) * inverse_diag[k]
            cur = cur - lower[k] * pivot_row
            inv_cols[j] = jnp.where(row == k, pivot_row, cur)

    def solve(i, x):
        total = inv_cols[0][:, 8 * i : 8 * i + 1] * x[0:1]
        for j in range(1, 8):
            total = total + inv_cols[j][:, 8 * i : 8 * i + 1] * x[j : j + 1]
        return total

    for m in range(2):
        for s in range(4):
            h_out[m, s] = solve(2 * s + m, p[s, m])

    counted(f.at[pl.ds(0, 63)], all_r).wait_recv()
    for m in range(2):
        for s in range(4):
            r_out[m, s] = solve(2 * s + m, jnp.concatenate([f[(s * NZ + j) * 2 + m] for j in range(NZ)], 1))

    counted(q.at[pl.ds(2, 2)], fac_s).wait_send()
    counted(own, own_s).wait_send()
    counted(c.at[pl.ds(0, 63)], sum_s).wait_send()
    counted(f.at[pl.ds(0, 63)], all_s).wait_send()
    counted(g1.at[pl.ds(0, NY - 1)], g1_s).wait_send()
    counted(g2.at[pl.ds(0, NZ - 1)], g2_s).wait_send()
    counted(g3.at[pl.ds(0, 2)], g3_s).wait_send()


COLUMNS = 256


def mix(w_ref, h_ref, r_ref, out_hbm, nx_hbm, ny_hbm, ov, out_sem, small_sem):
    stores = []
    for m in range(2):
        stores.append(pltpu.make_async_copy(r_ref.at[m, 2], nx_hbm.at[m], small_sem.at[m]))
        stores.append(pltpu.make_async_copy(r_ref.at[m, 3], ny_hbm.at[m], small_sem.at[2 + m]))
    for store in stores:
        store.start()
    for m in range(2):
        hh, hl, _ = split3(h_ref[m].reshape(32, 256))
        left = jnp.concatenate([hh, hh, hl], 0)
        for i in range(1024 // COLUMNS):
            part = pl.ds(i * COLUMNS, COLUMNS)
            rh, rl, _ = split3(r_ref[m, :, :, part].reshape(32, COLUMNS))
            right = jnp.concatenate([rh, rl, rh], 0)
            term = lax.dot_general(left, right, (((0,), (0,)), ((), ())), preferred_element_type=F32)
            n = m * (1024 // COLUMNS) + i
            ov[n] = w_ref[m, :, part] - 0.2 * term
            store = pltpu.make_async_copy(ov.at[n], out_hbm.at[m, :, part], out_sem.at[n])
            store.start()
            stores.append(store)
    for store in stores:
        store.wait()


def per_device(weights, factors_rx, factors_ry):
    w = weights.reshape(2, 256, 1024)
    vm = pltpu.VMEM
    dma = pltpu.SemaphoreType.DMA
    anyspec = pl.BlockSpec(memory_space=pl.ANY)
    hbm = pl.BlockSpec(memory_space=pltpu.HBM)
    vmem = pl.BlockSpec(memory_space=pltpu.VMEM)
    tile = (8, 128)
    r, h = pl.pallas_call(
        gossip,
        out_shape=(
            jax.ShapeDtypeStruct((2, 4, 8, 1024), F32),
            jax.ShapeDtypeStruct((2, 4, 8, 256), F32),
        ),
        in_specs=[hbm] * 3,
        out_specs=(vmem, vmem),
        scratch_shapes=[
            vm((4, 2, 8, 1024), F32),
            vm((2, 256, 1024), F32),
            vm((2, 256, 1024), BF16),
            vm((2, 256, 1024), BF16),
            vm((2, 256, 1024), BF16),
            vm((2, 1024, 256), BF16),
            vm((2, 1024, 256), BF16),
            vm((2, 1024, 256), BF16),
            vm((4, 2, 8, 256), F32),
            vm((4, 2, 8, 256), F32),
            vm((4, 2, 8, 256), F32),
            vm((64, *tile), F32),
            vm((64, *tile), F32),
            vm((NY, *tile), F32),
            vm((NZ, *tile), F32),
            vm((3, *tile), F32),
            vm((64, *tile), F32),
            dma((4,)),
            dma, dma,
            dma, dma((2,)),
            dma, dma,
            dma, dma,
            dma, dma,
            dma, dma,
            dma, dma,
            pltpu.SemaphoreType.REGULAR((3,)),
        ],
        compiler_params=pltpu.CompilerParams(
            collective_id=0, has_side_effects=True, vmem_limit_bytes=24 * 1024 * 1024
        ),
        name="gossip",
    )(*[pltpu.with_memory_space_constraint(x, pltpu.HBM) for x in (w, factors_rx.reshape(2, 8, 1024), factors_ry.reshape(2, 8, 1024))])
    mixed, next_rx, next_ry = pl.pallas_call(
        mix,
        out_shape=(
            jax.ShapeDtypeStruct((2, 256, 1024), F32),
            jax.ShapeDtypeStruct((2, 8, 1024), F32),
            jax.ShapeDtypeStruct((2, 8, 1024), F32),
        ),
        in_specs=[vmem, vmem, vmem],
        out_specs=(anyspec, anyspec, anyspec),
        scratch_shapes=[
            vm((2048 // COLUMNS, 256, COLUMNS), F32),
            dma((2048 // COLUMNS,)),
            dma((4,)),
        ],
        compiler_params=pltpu.CompilerParams(vmem_limit_bytes=24 * 1024 * 1024),
        name="mix",
    )(w, h, r)
    return (
        mixed.reshape(1, 1, 2, 256, 1024),
        next_rx.reshape(1, 1, 2, 8, 1024),
        next_ry.reshape(1, 1, 2, 8, 1024),
    )


def solution(mesh):
    wide = P("rx", "ry", None, "tp", None)
    narrow = P("rx", "ry", None, None, None)
    return jax.shard_map(
        per_device, mesh=mesh, in_specs=(wide, narrow, narrow), out_specs=(wide, narrow, narrow), check_vma=False
    )
```
